256 devices in a mesh: gx: 8 (over y, core), gy: 2 (over x_hi), ta: 16 (over z, x_lo).
Axes of the slice: x: 4 (x_hi: 2, x_lo: 2; x = x_hi * 2 + x_lo), y: 4, z: 8, core: 2. Of those that a mesh axis runs over, the one named last changes fastest.
Arguments:
- link_x: float32 [2, 3, 3, 32, 64, 256], P(None, None, None, 'gx', 'ta', 'gy'), may hold values from -1 to 1, as said below
- link_t: float32 [2, 3, 3, 32, 64, 256], P(None, None, None, 'gx', 'ta', 'gy'), may hold values from -1 to 1, as said below
Outputs:
- loops: float32 [6, 6, 32, 64], P(None, None, 'gx', 'ta')
The draws below stay inside these ranges and needn't reach their ends.
Inputs may be any that keep to these rules, and one draw needn't show every extreme that they name: `link_x`: every link matrix is special unitary. `link_t`: every link matrix is special unitary.
All inputs are finite; a program needn't handle non-finite values.
Results may differ from the reference program's by a relative error of at most 0.0001.
Values sent between devices are 32-bit elements; how exact they have to be, the bound alone decides.
A program may use at most 128 MiB of HBM per device.

```python
import jax
import jax.numpy as jnp

RMAX = 6
TMAX = 6
NX = 32
NT = 64
SPECT = 256


def complex_times(left_mat, right_mat):
    real_rows = []
    imag_rows = []
    for i in range(3):
        real_cols = []
        imag_cols = []
        for k in range(3):
            real_sum = left_mat[0][i][0] * right_mat[0][0][k] - left_mat[1][i][0] * right_mat[1][0][k]
            imag_sum = left_mat[0][i][0] * right_mat[1][0][k] + left_mat[1][i][0] * right_mat[0][0][k]
            for j in range(1, 3):
                real_sum = real_sum + left_mat[0][i][j] * right_mat[0][j][k] - left_mat[1][i][j] * right_mat[1][j][k]
                imag_sum = imag_sum + left_mat[0][i][j] * right_mat[1][j][k] + left_mat[1][i][j] * right_mat[0][j][k]
            real_cols.append(real_sum)
            imag_cols.append(imag_sum)
        real_rows.append(real_cols)
        imag_rows.append(imag_cols)
    return [real_rows, imag_rows]


def embed(theta, phi, psi, first, second):
    ones = jnp.ones_like(theta)
    zeros = jnp.zeros_like(theta)
    real_rows = [[ones if i == k else zeros for k in range(3)] for i in range(3)]
    imag_rows = [[zeros for k in range(3)] for i in range(3)]
    cos_t = jnp.cos(theta)
    sin_t = jnp.sin(theta)
    real_rows[first][first] = cos_t * jnp.cos(phi)
    imag_rows[first][first] = cos_t * jnp.sin(phi)
    real_rows[second][second] = cos_t * jnp.cos(phi)
    imag_rows[second][second] = -cos_t * jnp.sin(phi)
    real_rows[first][second] = sin_t * jnp.cos(psi)
    imag_rows[first][second] = sin_t * jnp.sin(psi)
    real_rows[second][first] = -sin_t * jnp.cos(psi)
    imag_rows[second][first] = sin_t * jnp.sin(psi)
    return [real_rows, imag_rows]


def near_identity(key):
    site_shape = (3, NX, NT, SPECT)
    keys = jax.random.split(key, 3)
    theta = jnp.clip(jax.random.normal(keys[0], site_shape, jnp.float32) * 0.35, -1.2, 1.2)
    phi = jnp.clip(jax.random.normal(keys[1], site_shape, jnp.float32) * 0.35, -1.2, 1.2)
    psi = jax.random.uniform(keys[2], site_shape, jnp.float32, -3.14159265, 3.14159265)
    result = embed(theta[0], phi[0], psi[0], 0, 1)
    result = complex_times(result, embed(theta[1], phi[1], psi[1], 1, 2))
    result = complex_times(result, embed(theta[2], phi[2], psi[2], 0, 2))
    real_part = jnp.stack([jnp.stack(row) for row in result[0]])
    imag_part = jnp.stack([jnp.stack(row) for row in result[1]])
    return jnp.stack([real_part, imag_part])


def draw_link_x(key, part):
    return near_identity(jax.random.fold_in(key, 11))


def draw_link_t(key, part):
    return near_identity(jax.random.fold_in(key, 23))


def setup_inputs(seed: int = 0) -> dict:
    splits = jax.random.split(jax.random.key(seed), 3)
    return {
        "link_x": draw_link_x(jax.random.fold_in(splits[2], 71), 0),
        "link_t": draw_link_t(jax.random.fold_in(splits[2], 71), 0),
    }


def times(left_mat, right_mat):
    real_rows = []
    imag_rows = []
    for i in range(3):
        real_cols = []
        imag_cols = []
        for k in range(3):
            real_sum = left_mat[0, i, 0] * right_mat[0, 0, k] - left_mat[1, i, 0] * right_mat[1, 0, k]
            imag_sum = left_mat[0, i, 0] * right_mat[1, 0, k] + left_mat[1, i, 0] * right_mat[0, 0, k]
            for j in range(1, 3):
                real_sum = real_sum + left_mat[0, i, j] * right_mat[0, j, k] - left_mat[1, i, j] * right_mat[1, j, k]
                imag_sum = imag_sum + left_mat[0, i, j] * right_mat[1, j, k] + left_mat[1, i, j] * right_mat[0, j, k]
            real_cols.append(real_sum)
            imag_cols.append(imag_sum)
        real_rows.append(jnp.stack(real_cols))
        imag_rows.append(jnp.stack(imag_cols))
    return jnp.stack([jnp.stack(real_rows), jnp.stack(imag_rows)])


def correlation(upper_half, lower_half):
    return jnp.sum(upper_half * lower_half, axis=(0, 1, 2, 5))


def reference(link_x, link_t):
    temporal = [link_t]
    factor = link_t
    for extent in range(1, TMAX):
        factor = jnp.roll(factor, -1, axis=4)
        temporal.append(times(temporal[-1], factor))
    carried = list(temporal)
    spatial = link_x
    factor_x = link_x
    all_rows = []
    for radius in range(RMAX):
        if radius > 0:
            factor_x = jnp.roll(factor_x, -1, axis=3)
            spatial = times(spatial, factor_x)
        carried = [jnp.roll(field, -1, axis=3) for field in carried]
        shifted = spatial
        row_sums = []
        for extent in range(TMAX):
            shifted = jnp.roll(shifted, -1, axis=4)
            upper_half = times(spatial, carried[extent])
            lower_half = times(temporal[extent], shifted)
            row_sums.append(correlation(upper_half, lower_half))
        all_rows.append(jnp.stack(row_sums))
    return jnp.stack(all_rows) / (3.0 * SPECT)
```

```python
import jax
import jax.numpy as jnp
from jax import lax
from jax.experimental import pallas as pl
from jax.experimental.pallas import tpu as pltpu
from jax.sharding import PartitionSpec as P

RMAX = 6
TMAX = 6
MESH = pl.DeviceIdType.MESH

V_COPIES = ((1, 0, 2), (0, 1, 2), (1, 1, 2), (0, 2, 1), (1, 2, 1))
E_COPIES = (
    (1, 0, 1, 3),
    (2, 0, 0, 3),
    (0, 1, 2, 3),
    (1, 1, 1, 3),
    (2, 1, 0, 3),
    (1, 2, 1, 2),
    (2, 2, 0, 2),
)
PARTNERS = tuple((a, g) for a in range(3) for g in range(3) if a or g)


def cmul(a, b):
    return a[0] * b[0] - a[1] * b[1], a[0] * b[1] + a[1] * b[0]


def cmul_conj(a, b):
    return a[0] * b[0] + a[1] * b[1], a[1] * b[0] - a[0] * b[1]


def csum(terms):
    real, imag = terms[0]
    for term in terms[1:]:
        real, imag = real + term[0], imag + term[1]
    return real, imag


def matmul(a, b):
    return [[csum([cmul(row[j], b[j][k]) for j in range(3)]) for k in range(3)] for row in a]


def matmul_dagger(a, b):
    return [[csum([cmul_conj(row[j], b[k][j]) for j in range(3)]) for k in range(3)] for row in a]


def third_row(a):
    row = []
    for i in range(3):
        j, k = (i + 1) % 3, (i + 2) % 3
        first = cmul(a[0][j], a[1][k])
        second = cmul(a[0][k], a[1][j])
        row.append((first[0] - second[0], second[1] - first[1]))
    return [a[0], a[1], row]


def per_element(function, *matrices):
    return [
        [tuple(function(*(m[i][j][c] for m in matrices)) for c in range(2)) for j in range(3)]
        for i in range(len(matrices[0]))
    ]


def load(ref, lead, rows, window=slice(None)):
    return [
        [tuple(ref[(*lead, c * 3 * rows + i * 3 + j, window)] for c in range(2)) for j in range(3)]
        for i in range(rows)
    ]


def store(ref, lead, matrix, rows, window=slice(None)):
    for c in range(2):
        for i in range(rows):
            for j in range(3):
                ref[(*lead, c * 3 * rows + i * 3 + j, window)] = matrix[i][j][c]


def roll(value, shift):
    shift = shift % 8
    return value if shift == 0 else pltpu.roll(value, shift, 0)


def kernel(
    sizes, link_x, link_t, out, ux, ut, field, edge, left, right, tiles, chain, tmp, part, peer,
    in_sem, v_send, v_recv, e_send, e_recv, sum_send, sum_recv,
):
    n_x, n_y, n_t = sizes
    x_at, y_at, t_at = lax.axis_index("gx"), lax.axis_index("gy"), lax.axis_index("ta")
    other_y = lax.rem(y_at + 1, n_y)

    barrier = pltpu.get_barrier_semaphore()
    for a, g in PARTNERS:
        above = {"gx": lax.rem(x_at + g, n_x), "ta": lax.rem(t_at + a, n_t)}
        pl.semaphore_signal(barrier, inc=1, device_id=above, device_id_type=MESH)
    pl.semaphore_signal(barrier, inc=1, device_id={"gy": other_y}, device_id_type=MESH)

    copy_x = pltpu.make_async_copy(link_x, ux, in_sem.at[0])
    copy_t = pltpu.make_async_copy(link_t, ut, in_sem.at[1])
    copy_x.start()
    copy_t.start()

    row = lax.broadcasted_iota(jnp.int32, (8, 128), 0)
    time = lax.rem(row, 4)
    lower = row < 4
    one = jnp.ones((8, 128), jnp.float32)
    zero = jnp.zeros((8, 128), jnp.float32)
    unit = [[(one if i == k else zero, zero) for k in range(3)] for i in range(3)]

    def pick(mask, a, b):
        return per_element(lambda p, q: jnp.where(mask, p, q), a, b)

    def rolled(a, shift):
        return per_element(lambda p: roll(p, shift), a)

    copy_x.wait()
    u0 = load(ux, (), 3, pl.ds(0, 8))
    u1 = load(ux, (), 3, pl.ds(8, 8))
    halves = matmul(pick(lower, u0, rolled(u1, 4)), pick(lower, rolled(u0, 4), u1))
    whole = matmul(pick(lower, halves, rolled(halves, 4)), pick(lower, u1, halves))
    starts = [
        pick(lower, unit, rolled(u0, 4)),
        pick(lower, halves, rolled(whole, 4)),
    ]
    store(edge, (0, 0, 2), per_element(lambda p: p[4:8], whole[:2]), 2)
    copy_t.wait()
    links = []
    for xp in range(2):
        begin = starts[xp]
        end = pick(time == 3, unit, rolled(begin, 7))
        v = matmul_dagger(matmul(begin[:2], load(ut, (), 3, pl.ds(8 * xp, 8))), end)
        store(field, (0, xp), v, 2)
        links.append(v)

    def first_times(low, high):
        value = jnp.where(row == 0, low, roll(low, -3))
        value = jnp.where(row == 2, roll(high, 2), value)
        return jnp.where(row == 3, roll(high, -1), value)[0:4]

    store(edge, (0, 0, 0), per_element(first_times, links[0], links[1]), 2)
    store(edge, (0, 0, 1), per_element(first_times, starts[0][:2], starts[1][:2]), 2)

    pl.semaphore_wait(barrier, len(PARTNERS) + 1)

    v_copies, e_copies = {}, {}
    order = [("e", i) for i in range(len(E_COPIES))] + [("v", i) for i in range(len(V_COPIES))]
    for kind, i in order:
        a, g = (V_COPIES if kind == "v" else E_COPIES)[i][:2]
        below = {"gx": lax.rem(x_at + n_x - g, n_x), "ta": lax.rem(t_at + n_t - a, n_t)}
        if kind == "v":
            pairs = V_COPIES[i][2]
            copy = pltpu.make_async_remote_copy(
                src_ref=field.at[0, pl.ds(0, pairs)],
                dst_ref=field.at[a, pl.ds(2 * g, pairs)],
                send_sem=v_send.at[i],
                recv_sem=v_recv.at[i],
                device_id=below,
                device_id_type=MESH,
            )
            v_copies[a, g] = copy
        else:
            first, last = E_COPIES[i][2:]
            copy = pltpu.make_async_remote_copy(
                src_ref=edge.at[0, 0, pl.ds(first, last - first)],
                dst_ref=edge.at[a, g, pl.ds(first, last - first)],
                send_sem=e_send.at[i],
                recv_sem=e_recv.at[i],
                device_id=below,
                device_id_type=MESH,
            )
            e_copies[a, g] = copy
        copy.start()

    def arrived(g):
        for copies in (e_copies, v_copies):
            for a in range(3):
                if (a, g) in copies:
                    copies[a, g].wait_recv()

    def both_halves(a, g):
        value = load(edge, (a, g, 2), 2)
        store(tmp, (), value, 2, pl.ds(0, 4))
        store(tmp, (), value, 2, pl.ds(4, 4))
        return third_row(load(tmp, (), 2))

    def spread(matrix, rows, first):
        return per_element(lambda p: jnp.broadcast_to(p[first : first + 1], (8, 128)), matrix[:rows])

    def change_of_gauge(g):
        previous = None
        for a in (2, 1, 0):
            value = both_halves(a, 0)
            if g == 2:
                if a == 2:
                    value = matmul(value, both_halves(2, 1))
                else:
                    value = matmul(value, both_halves(a, 1))
            if a == 2:
                store(left, (2,), spread(value, 2, 0), 2)
                store(right, (2,), spread(value, 3, 1), 3)
            else:
                store(left, (a,), value[:2], 2)
                after = pick(time == 3, previous, rolled(value, 7))
                store(right, (a,), after, 3)
            previous = spread(value, 3, 0)

    def row_pair(a, g, piece, q):
        low = load(edge, (a, g, piece), 2, pl.ds(2 * q, 1))
        high = load(edge, (a, g, piece), 2, pl.ds(2 * q + 1, 1))
        wide = lambda p: jnp.broadcast_to(p, (8, 128))
        return third_row(per_element(lambda p, s: jnp.where(lower, wide(p), wide(s)), low, high))

    def into_window(value, a, g):
        if g > 0:
            value = third_row(matmul_dagger(value, load(right, (a,), 3)))
            value = matmul(load(left, (a,), 2), value)
        return third_row(value)

    def pair(g, q):
        xp = 2 * g + q
        for a in range(2):
            fix = pick(time == 3, row_pair(a + 1, g, 1, q), unit)
            value = matmul_dagger(load(field, (a, xp), 2), fix)
            store(tiles, (a,), into_window(value, a, g), 3)
        store(tiles, (2,), into_window(row_pair(2, g, 0, q)[:2], 2, g), 3)
        product = load(tiles, (0,), 3)
        store(chain, (0, xp), product, 3)
        for k in range(1, TMAX):
            if k < 4:
                here, after = load(tiles, (0,), 3), load(tiles, (1,), 3)
                factor = pick(time < 4 - k, rolled(here, -k), rolled(after, 4 - k))
            elif k == 4:
                factor = load(tiles, (1,), 3)
            else:
                factor = pick(time < 3, rolled(load(tiles, (1,), 3), -1), load(tiles, (2,), 3))
            product = third_row(matmul(product[:2], factor))
            store(chain, (k, xp), product, 3)

    for g in range(3):
        arrived(g)
        if g > 0:
            change_of_gauge(g)

        def body(q, carry, g=g):
            pair(g, q)
            return carry

        lax.fori_loop(0, 2 if g < 2 else 1, body, 0)

    lane = lax.broadcasted_iota(jnp.int32, (8, 128), 1)

    def correlate(u, sums):
        totals = [None] * (2 * RMAX)
        for c in range(18):
            even = [chain[u, m, c] for m in range(5)]
            turned = [roll(value, 4) for value in even]
            odd = [jnp.where(lower, turned[m], turned[m + 1]) for m in range(4)]
            for r in range(1, RMAX + 1):
                for xp in range(2):
                    far = odd[xp + r // 2] if r % 2 else even[xp + r // 2]
                    i = 2 * (r - 1) + xp
                    term = even[xp] * far
                    totals[i] = term if totals[i] is None else totals[i] + term
        for i in range(2 * RMAX):
            total = jnp.sum(totals[i], axis=1, keepdims=True)
            sums = jnp.where(lane == u * (2 * RMAX) + i, total, sums)
        return sums

    part[...] = lax.fori_loop(0, TMAX, correlate, zero)

    for copies in (e_copies, v_copies):
        for copy in copies.values():
            copy.wait_send()
    swap = pltpu.make_async_remote_copy(
        src_ref=part,
        dst_ref=peer,
        send_sem=sum_send,
        recv_sem=sum_recv,
        device_id={"gy": other_y},
        device_id_type=MESH,
    )
    swap.start()
    swap.wait()
    out[...] = (part[...] + peer[...]) / (3.0 * 128 * n_y)


def solution(mesh):
    sizes = tuple(mesh.shape[name] for name in ("gx", "gy", "ta"))

    def local(link_x, link_t):
        vmem = lambda *shape: pltpu.VMEM(shape, jnp.float32)
        sums = pl.pallas_call(
            lambda *refs: kernel(sizes, *refs),
            out_shape=jax.ShapeDtypeStruct((8, 128), jnp.float32),
            in_specs=[pl.BlockSpec(memory_space=pl.ANY)] * 2,
            out_specs=pl.BlockSpec(memory_space=pltpu.VMEM),
            scratch_shapes=[
                vmem(18, 16, 128),
                vmem(18, 16, 128),
                vmem(2, 5, 12, 8, 128),
                vmem(3, 3, 3, 12, 4, 128),
                vmem(3, 12, 8, 128),
                vmem(3, 18, 8, 128),
                vmem(3, 18, 8, 128),
                vmem(TMAX, 5, 18, 8, 128),
                vmem(12, 8, 128),
                vmem(8, 128),
                vmem(8, 128),
                pltpu.SemaphoreType.DMA((2,)),
                pltpu.SemaphoreType.DMA((len(V_COPIES),)),
                pltpu.SemaphoreType.DMA((len(V_COPIES),)),
                pltpu.SemaphoreType.DMA((len(E_COPIES),)),
                pltpu.SemaphoreType.DMA((len(E_COPIES),)),
                pltpu.SemaphoreType.DMA,
                pltpu.SemaphoreType.DMA,
            ],
            compiler_params=pltpu.CompilerParams(collective_id=0, has_side_effects=True),
        )(link_x.reshape(18, 16, 128), link_t.reshape(18, 16, 128))
        sums = sums[:, : 12 * TMAX].reshape(2, 4, TMAX, RMAX, 2)
        return sums.transpose(3, 2, 4, 0, 1).reshape(RMAX, TMAX, 4, 4)

    return jax.shard_map(
        local,
        mesh=mesh,
        in_specs=(P(None, None, None, "gx", "ta", "gy"),) * 2,
        out_specs=P(None, None, "gx", "ta"),
        check_vma=False,
    )
```

```python
import jax
import jax.numpy as jnp
from jax import lax
from jax.experimental import pallas as pl
from jax.experimental.pallas import tpu as pltpu
from jax.sharding import PartitionSpec as P

RMAX = 6
TMAX = 6
MESH = pl.DeviceIdType.MESH

V_COPIES = ((1, 0, 2), (0, 1, 2), (1, 1, 2), (0, 2, 1), (1, 2, 1))
E_COPIES = (
    (1, 0, 1, 3),
    (2, 0, 0, 3),
    (0, 1, 2, 3),
    (1, 1, 1, 3),
    (2, 1, 0, 3),
    (1, 2, 1, 2),
    (2, 2, 0, 2),
)
PARTNERS = tuple((a, g) for a in range(3) for g in range(3) if a or g)


def cmul(a, b):
    return a[0] * b[0] - a[1] * b[1], a[0] * b[1] + a[1] * b[0]


def cmul_conj(a, b):
    return a[0] * b[0] + a[1] * b[1], a[1] * b[0] - a[0] * b[1]


def csum(terms):
    real, imag = terms[0]
    for term in terms[1:]:
        real, imag = real + term[0], imag + term[1]
    return real, imag


def matmul(a, b):
    return [[csum([cmul(row[j], b[j][k]) for j in range(3)]) for k in range(3)] for row in a]


def matmul_dagger(a, b):
    return [[csum([cmul_conj(row[j], b[k][j]) for j in range(3)]) for k in range(3)] for row in a]


def third_row(a):
    row = []
    for i in range(3):
        j, k = (i + 1) % 3, (i + 2) % 3
        first = cmul(a[0][j], a[1][k])
        second = cmul(a[0][k], a[1][j])
        row.append((first[0] - second[0], second[1] - first[1]))
    return [a[0], a[1], row]


def per_element(function, *matrices):
    return [
        [tuple(function(*(m[i][j][c] for m in matrices)) for c in range(2)) for j in range(3)]
        for i in range(len(matrices[0]))
    ]


def load(ref, lead, rows, window=slice(None)):
    return [
        [tuple(ref[(*lead, c * 3 * rows + i * 3 + j, window)] for c in range(2)) for j in range(3)]
        for i in range(rows)
    ]


def store(ref, lead, matrix, rows, window=slice(None)):
    for c in range(2):
        for i in range(rows):
            for j in range(3):
                ref[(*lead, c * 3 * rows + i * 3 + j, window)] = matrix[i][j][c]


def roll(value, shift):
    shift = shift % 8
    return value if shift == 0 else pltpu.roll(value, shift, 0)


def kernel(
    sizes, link_x, link_t, out, ux, ut, field, edge, left, right, tiles, chain, tmp, part, peer,
    in_sem, ready, v_send, v_recv, e_send, e_recv, sum_send, sum_recv,
):
    n_x, n_y, n_t = sizes
    x_at, y_at, t_at = lax.axis_index("gx"), lax.axis_index("gy"), lax.axis_index("ta")
    other_y = lax.rem(y_at + 1, n_y)

    def above(a, g):
        return {"gx": lax.rem(x_at + g, n_x), "ta": lax.rem(t_at + a, n_t)}

    def below(a, g):
        return {"gx": lax.rem(x_at + n_x - g, n_x), "ta": lax.rem(t_at + n_t - a, n_t)}

    barrier = pltpu.get_barrier_semaphore()
    for a, g in PARTNERS:

        @pl.when(t_at + a < n_t)
        def _():
            pl.semaphore_signal(barrier, inc=1, device_id=above(a, g), device_id_type=MESH)

        @pl.when(t_at < a)
        def _():
            pl.semaphore_signal(barrier, inc=1, device_id=below(a, g), device_id_type=MESH)

    pl.semaphore_signal(barrier, inc=1, device_id={"gy": other_y}, device_id_type=MESH)

    copy_x = pltpu.make_async_copy(link_x, ux, in_sem.at[0])
    copy_t = pltpu.make_async_copy(link_t, ut, in_sem.at[1])
    copy_x.start()
    copy_t.start()

    row = lax.broadcasted_iota(jnp.int32, (8, 128), 0)
    time = lax.rem(row, 4)
    lower = row < 4
    one = jnp.ones((8, 128), jnp.float32)
    zero = jnp.zeros((8, 128), jnp.float32)
    unit = [[(one if i == k else zero, zero) for k in range(3)] for i in range(3)]

    def pick(mask, a, b):
        return per_element(lambda p, q: jnp.where(mask, p, q), a, b)

    def rolled(a, shift):
        return per_element(lambda p: roll(p, shift), a)

    copy_x.wait()
    u0 = load(ux, (), 3, pl.ds(0, 8))
    u1 = load(ux, (), 3, pl.ds(8, 8))
    halves = matmul(pick(lower, u0, rolled(u1, 4)), pick(lower, rolled(u0, 4), u1))
    whole = matmul(pick(lower, halves, rolled(halves, 4)), pick(lower, u1, halves))
    starts = [
        pick(lower, unit, rolled(u0, 4)),
        pick(lower, halves, rolled(whole, 4)),
    ]
    store(edge, (0, 0, 2), per_element(lambda p: p[4:8], whole[:2]), 2)
    copy_t.wait()
    links = []
    for xp in range(2):
        begin = starts[xp]
        end = pick(time == 3, unit, rolled(begin, 7))
        v = matmul_dagger(matmul(begin[:2], load(ut, (), 3, pl.ds(8 * xp, 8))), end)
        store(field, (0, xp), v, 2)
        links.append(v)

    def first_times(low, high):
        value = jnp.where(row == 0, low, roll(low, -3))
        value = jnp.where(row == 2, roll(high, 2), value)
        return jnp.where(row == 3, roll(high, -1), value)[0:4]

    store(edge, (0, 0, 0), per_element(first_times, links[0], links[1]), 2)
    store(edge, (0, 0, 1), per_element(first_times, starts[0][:2], starts[1][:2]), 2)

    peers = 1
    for a, _ in PARTNERS:
        peers += (t_at >= a).astype(jnp.int32) if a else 1
        peers += (t_at + a >= n_t).astype(jnp.int32) if a else 0
    pl.semaphore_wait(barrier, peers)

    for k, (a, g) in enumerate(PARTNERS):

        @pl.when(t_at + a >= n_t)
        def _():
            pl.semaphore_signal(ready.at[k], inc=1, device_id=above(a, g), device_id_type=MESH)


    v_copies, e_copies = {}, {}
    order = [("e", i) for i in range(len(E_COPIES))] + [("v", i) for i in range(len(V_COPIES))]
    for kind, i in order:
        a, g = (V_COPIES if kind == "v" else E_COPIES)[i][:2]
        if kind == "v":
            pairs = V_COPIES[i][2]
            copy = pltpu.make_async_remote_copy(
                src_ref=field.at[0, pl.ds(0, pairs)],
                dst_ref=field.at[a, pl.ds(2 * g, pairs)],
                send_sem=v_send.at[i],
                recv_sem=v_recv.at[i],
                device_id=below(a, g),
                device_id_type=MESH,
            )
            v_copies[a, g] = copy
        else:
            first, last = E_COPIES[i][2:]
            copy = pltpu.make_async_remote_copy(
                src_ref=edge.at[0, 0, pl.ds(first, last - first)],
                dst_ref=edge.at[a, g, pl.ds(first, last - first)],
                send_sem=e_send.at[i],
                recv_sem=e_recv.at[i],
                device_id=below(a, g),
                device_id_type=MESH,
            )
            e_copies[a, g] = copy
        if a:
            pl.when(t_at >= a)(copy.start)
        else:
            copy.start()

    for k, (a, g) in enumerate(PARTNERS):

        @pl.when(t_at < a)
        def _():
            pl.semaphore_wait(ready.at[k], 1)
            for copies in (e_copies, v_copies):
                if (a, g) in copies:
                    copies[a, g].start()

    def arrived(g):
        for copies in (e_copies, v_copies):
            for a in range(3):
                if (a, g) in copies:
                    copies[a, g].wait_recv()

    def both_halves(a, g):
        value = load(edge, (a, g, 2), 2)
        store(tmp, (), value, 2, pl.ds(0, 4))
        store(tmp, (), value, 2, pl.ds(4, 4))
        return third_row(load(tmp, (), 2))

    def spread(matrix, rows, first):
        return per_element(lambda p: jnp.broadcast_to(p[first : first + 1], (8, 128)), matrix[:rows])

    def change_of_gauge(g):
        previous = None
        for a in (2, 1, 0):
            value = both_halves(a, 0)
            if g == 2:
                if a == 2:
                    value = matmul(value, both_halves(2, 1))
                else:
                    value = matmul(value, both_halves(a, 1))
            if a == 2:
                store(left, (2,), spread(value, 2, 0), 2)
                store(right, (2,), spread(value, 3, 1), 3)
            else:
                store(left, (a,), value[:2], 2)
                after = pick(time == 3, previous, rolled(value, 7))
                store(right, (a,), after, 3)
            previous = spread(value, 3, 0)

    def row_pair(a, g, piece, q):
        low = load(edge, (a, g, piece), 2, pl.ds(2 * q, 1))
        high = load(edge, (a, g, piece), 2, pl.ds(2 * q + 1, 1))
        wide = lambda p: jnp.broadcast_to(p, (8, 128))
        return third_row(per_element(lambda p, s: jnp.where(lower, wide(p), wide(s)), low, high))

    def into_window(value, a, g):
        if g > 0:
            value = third_row(matmul_dagger(value, load(right, (a,), 3)))
            value = matmul(load(left, (a,), 2), value)
        return third_row(value)

    def pair(g, q):
        xp = 2 * g + q
        for a in range(2):
            fix = pick(time == 3, row_pair(a + 1, g, 1, q), unit)
            value = matmul_dagger(load(field, (a, xp), 2), fix)
            store(tiles, (a,), into_window(value, a, g), 3)
        store(tiles, (2,), into_window(row_pair(2, g, 0, q)[:2], 2, g), 3)
        product = load(tiles, (0,), 3)
        store(chain, (0, xp), product, 3)
        for k in range(1, TMAX):
            if k < 4:
                here, after = load(tiles, (0,), 3), load(tiles, (1,), 3)
                factor = pick(time < 4 - k, rolled(here, -k), rolled(after, 4 - k))
            elif k == 4:
                factor = load(tiles, (1,), 3)
            else:
                factor = pick(time < 3, rolled(load(tiles, (1,), 3), -1), load(tiles, (2,), 3))
            product = third_row(matmul(product[:2], factor))
            store(chain, (k, xp), product, 3)

    lane = lax.broadcasted_iota(jnp.int32, (8, 128), 1)

    def correlate(sums, picked):
        def body(u, sums):
            totals = {}
            for c in range(18):
                tile = {}

                def even(m):
                    if m not in tile:
                        tile[m] = chain[u, m, c]
                    return tile[m]

                def turned(m):
                    if ("t", m) not in tile:
                        tile["t", m] = roll(even(m), 4)
                    return tile["t", m]

                def odd(m):
                    if ("o", m) not in tile:
                        tile["o", m] = jnp.where(lower, turned(m), turned(m + 1))
                    return tile["o", m]

                for r, xp in picked:
                    far = odd(xp + r // 2) if r % 2 else even(xp + r // 2)
                    term = even(xp) * far
                    totals[r, xp] = totals[r, xp] + term if (r, xp) in totals else term
            for r, xp in picked:
                total = jnp.sum(totals[r, xp], axis=1, keepdims=True)
                sums = jnp.where(lane == 8 * (2 * (r - 1) + xp) + u, total, sums)
            return sums

        return lax.fori_loop(0, TMAX, body, sums)

    def chains(g):
        def body(q, carry):
            pair(g, q)
            return carry

        lax.fori_loop(0, 2 if g < 2 else 1, body, 0)

    loops = [(r, xp) for r in range(1, RMAX + 1) for xp in range(2)]
    last = [(r, xp) for r, xp in loops if xp + (r + 1) // 2 == 4]
    arrived(0)
    change_of_gauge(1)
    chains(0)
    arrived(1)
    chains(1)
    change_of_gauge(2)
    sums = correlate(zero, [loop for loop in loops if loop not in last])
    arrived(2)
    chains(2)
    part[...] = correlate(sums, last)

    for copies in (e_copies, v_copies):
        for copy in copies.values():
            copy.wait_send()
    swap = pltpu.make_async_remote_copy(
        src_ref=part,
        dst_ref=peer,
        send_sem=sum_send,
        recv_sem=sum_recv,
        device_id={"gy": other_y},
        device_id_type=MESH,
    )
    swap.start()
    swap.wait()
    sums = (part[...] + peer[...]) / (3.0 * 128 * n_y)
    for r, xp in loops:
        at = 8 * (2 * (r - 1) + xp)
        value = sums if at == 0 else pltpu.roll(sums, 128 - at, 1)
        out[r - 1, 2 * xp] = value[0:4, 0:TMAX]
        out[r - 1, 2 * xp + 1] = value[4:8, 0:TMAX]


def solution(mesh):
    sizes = tuple(mesh.shape[name] for name in ("gx", "gy", "ta"))

    def local(link_x, link_t):
        vmem = lambda *shape: pltpu.VMEM(shape, jnp.float32)
        sums = pl.pallas_call(
            lambda *refs: kernel(sizes, *refs),
            out_shape=jax.ShapeDtypeStruct((RMAX, 4, 4, TMAX), jnp.float32),
            in_specs=[pl.BlockSpec(memory_space=pl.ANY)] * 2,
            out_specs=pl.BlockSpec(memory_space=pltpu.VMEM),
            scratch_shapes=[
                vmem(18, 16, 128),
                vmem(18, 16, 128),
                vmem(2, 5, 12, 8, 128),
                vmem(3, 3, 3, 12, 4, 128),
                vmem(3, 12, 8, 128),
                vmem(3, 18, 8, 128),
                vmem(3, 18, 8, 128),
                vmem(TMAX, 5, 18, 8, 128),
                vmem(12, 8, 128),
                vmem(8, 128),
                vmem(8, 128),
                pltpu.SemaphoreType.DMA((2,)),
                pltpu.SemaphoreType.REGULAR((len(PARTNERS),)),
                pltpu.SemaphoreType.DMA((len(V_COPIES),)),
                pltpu.SemaphoreType.DMA((len(V_COPIES),)),
                pltpu.SemaphoreType.DMA((len(E_COPIES),)),
                pltpu.SemaphoreType.DMA((len(E_COPIES),)),
                pltpu.SemaphoreType.DMA,
                pltpu.SemaphoreType.DMA,
            ],
            compiler_params=pltpu.CompilerParams(collective_id=0, has_side_effects=True),
        )(link_x.reshape(18, 16, 128), link_t.reshape(18, 16, 128))
        return sums.transpose(0, 3, 1, 2)

    return jax.shard_map(
        local,
        mesh=mesh,
        in_specs=(P(None, None, None, "gx", "ta", "gy"),) * 2,
        out_specs=P(None, None, "gx", "ta"),
        check_vma=False,
    )
```

```python
import jax
import jax.numpy as jnp
from jax import lax
from jax.experimental import pallas as pl
from jax.experimental.pallas import tpu as pltpu
from jax.sharding import PartitionSpec as P

RMAX = 6
TMAX = 6
MESH = pl.DeviceIdType.MESH

V_COPIES = ((1, 0, 2), (0, 1, 2), (1, 1, 2), (0, 2, 1), (1, 2, 1))
E_COPIES = (
    (1, 0, 1, 3),
    (2, 0, 0, 3),
    (0, 1, 2, 3),
    (1, 1, 1, 3),
    (2, 1, 0, 3),
    (1, 2, 1, 2),
    (2, 2, 0, 2),
)
PARTNERS = tuple((a, g) for a in range(3) for g in range(3) if a or g)


def cmul(a, b):
    return a[0] * b[0] - a[1] * b[1], a[0] * b[1] + a[1] * b[0]


def cmul_conj(a, b):
    return a[0] * b[0] + a[1] * b[1], a[1] * b[0] - a[0] * b[1]


def csum(terms):
    real, imag = terms[0]
    for term in terms[1:]:
        real, imag = real + term[0], imag + term[1]
    return real, imag


def matmul(a, b):
    return [[csum([cmul(row[j], b[j][k]) for j in range(3)]) for k in range(3)] for row in a]


def matmul_dagger(a, b):
    return [[csum([cmul_conj(row[j], b[k][j]) for j in range(3)]) for k in range(3)] for row in a]


def third_row(a):
    row = []
    for i in range(3):
        j, k = (i + 1) % 3, (i + 2) % 3
        first = cmul(a[0][j], a[1][k])
        second = cmul(a[0][k], a[1][j])
        row.append((first[0] - second[0], second[1] - first[1]))
    return [a[0], a[1], row]


def per_element(function, *matrices):
    return [
        [tuple(function(*(m[i][j][c] for m in matrices)) for c in range(2)) for j in range(3)]
        for i in range(len(matrices[0]))
    ]


def load(ref, lead, rows, window=slice(None)):
    return [
        [tuple(ref[(*lead, c * 3 * rows + i * 3 + j, window)] for c in range(2)) for j in range(3)]
        for i in range(rows)
    ]


def store(ref, lead, matrix, rows, window=slice(None)):
    for c in range(2):
        for i in range(rows):
            for j in range(3):
                ref[(*lead, c * 3 * rows + i * 3 + j, window)] = matrix[i][j][c]


def roll(value, shift):
    shift = shift % 8
    return value if shift == 0 else pltpu.roll(value, shift, 0)


def kernel(
    sizes, link_x, link_t, out, ux, ut, field, edge, left, right, tiles, chain, tmp, part, peer,
    in_sem, ready, y_ready, v_send, v_recv, v_pass, e_send, e_recv, e_pass, sum_send, sum_recv,
):
    n_x, n_y, n_t = sizes
    x_at, y_at, t_at = lax.axis_index("gx"), lax.axis_index("gy"), lax.axis_index("ta")
    other_y = lax.rem(y_at + 1, n_y)

    def above(a, g):
        return {"gx": lax.rem(x_at + g, n_x), "ta": lax.rem(t_at + a, n_t)}

    def below(a, g):
        return {"gx": lax.rem(x_at + n_x - g, n_x), "ta": lax.rem(t_at + n_t - a, n_t)}

    barrier = pltpu.get_barrier_semaphore()
    def always(*conditions):
        known = [c for c in conditions if isinstance(c, bool)]
        traced = [c for c in conditions if not isinstance(c, bool)]
        if not all(known):
            return False
        result = True
        for c in traced:
            result = c if result is True else result & c
        return result

    def when(condition, action):
        if condition is True:
            action()
        elif condition is not False:
            pl.when(condition)(action)

    odd = lax.rem(x_at, 2) == 1
    even = lax.rem(x_at, 2) == 0

    def sends(a, g):
        return odd if g == 2 else even if g == 1 and a > 0 else True

    def receives(a, g):
        return odd if g == 2 or (g == 1 and a > 0) else True

    def sends_over_end(a, g):
        return (t_at < a) | (x_at < g)

    def receives_over_end(a, g):
        return (t_at + a >= n_t) | (x_at + g >= n_x)

    peers = (y_at > 0).astype(jnp.int32)
    for a, g in PARTNERS:

        @pl.when(always(receives(a, g), jnp.logical_not(receives_over_end(a, g))))
        def _():
            pl.semaphore_signal(barrier, inc=1, device_id=above(a, g), device_id_type=MESH)

        @pl.when(always(sends(a, g), sends_over_end(a, g)))
        def _():
            pl.semaphore_signal(barrier, inc=1, device_id=below(a, g), device_id_type=MESH)

        peers += always(sends(a, g), jnp.logical_not(sends_over_end(a, g))).astype(jnp.int32)
        peers += always(receives(a, g), receives_over_end(a, g)).astype(jnp.int32)

    @pl.when(y_at == 0)
    def _():
        pl.semaphore_signal(barrier, inc=1, device_id={"gy": other_y}, device_id_type=MESH)

    copy_x = pltpu.make_async_copy(link_x, ux, in_sem.at[0])
    copy_t = pltpu.make_async_copy(link_t, ut, in_sem.at[1])
    copy_x.start()
    copy_t.start()

    row = lax.broadcasted_iota(jnp.int32, (8, 128), 0)
    time = lax.rem(row, 4)
    lower = row < 4
    one = jnp.ones((8, 128), jnp.float32)
    zero = jnp.zeros((8, 128), jnp.float32)
    unit = [[(one if i == k else zero, zero) for k in range(3)] for i in range(3)]

    def pick(mask, a, b):
        return per_element(lambda p, q: jnp.where(mask, p, q), a, b)

    def rolled(a, shift):
        return per_element(lambda p: roll(p, shift), a)

    copy_x.wait()
    u0 = load(ux, (), 3, pl.ds(0, 8))
    u1 = load(ux, (), 3, pl.ds(8, 8))
    halves = matmul(pick(lower, u0, rolled(u1, 4)), pick(lower, rolled(u0, 4), u1))
    whole = matmul(pick(lower, halves, rolled(halves, 4)), pick(lower, u1, halves))
    starts = [
        pick(lower, unit, rolled(u0, 4)),
        pick(lower, halves, rolled(whole, 4)),
    ]
    store(edge, (0, 0, 2), per_element(lambda p: p[4:8], whole[:2]), 2)
    copy_t.wait()
    links = []
    for xp in range(2):
        begin = starts[xp]
        end = pick(time == 3, unit, rolled(begin, 7))
        v = matmul_dagger(matmul(begin[:2], load(ut, (), 3, pl.ds(8 * xp, 8))), end)
        store(field, (0, xp), v, 2)
        links.append(v)

    def first_times(low, high):
        value = jnp.where(row == 0, low, roll(low, -3))
        value = jnp.where(row == 2, roll(high, 2), value)
        return jnp.where(row == 3, roll(high, -1), value)[0:4]

    store(edge, (0, 0, 0), per_element(first_times, links[0], links[1]), 2)
    store(edge, (0, 0, 1), per_element(first_times, starts[0][:2], starts[1][:2]), 2)


    @pl.when(peers > 0)
    def _():
        pl.semaphore_wait(barrier, peers)

    for k, (a, g) in enumerate(PARTNERS):

        @pl.when(always(receives(a, g), receives_over_end(a, g)))
        def _():
            pl.semaphore_signal(ready.at[k], inc=1, device_id=above(a, g), device_id_type=MESH)

    @pl.when(y_at > 0)
    def _():
        pl.semaphore_signal(y_ready, inc=1, device_id={"gy": other_y}, device_id_type=MESH)

    def v_copy(i, a, g, target, send_sem):
        to_a, to_g, pairs = V_COPIES[i]
        return pltpu.make_async_remote_copy(
            src_ref=field.at[a, pl.ds(2 * g, pairs)],
            dst_ref=field.at[to_a, pl.ds(2 * to_g, pairs)],
            send_sem=send_sem.at[i],
            recv_sem=v_recv.at[i],
            device_id=target,
            device_id_type=MESH,
        )

    def e_copy(i, a, g, target, send_sem):
        to_a, to_g, first, last = E_COPIES[i]
        return pltpu.make_async_remote_copy(
            src_ref=edge.at[a, g, pl.ds(first, last - first)],
            dst_ref=edge.at[to_a, to_g, pl.ds(first, last - first)],
            send_sem=send_sem.at[i],
            recv_sem=e_recv.at[i],
            device_id=target,
            device_id_type=MESH,
        )

    copies = {partner: [] for partner in PARTNERS}
    passed_on = {partner: [] for partner in PARTNERS}
    for make, table, own_sem, pass_sem in (
        (e_copy, E_COPIES, e_send, e_pass),
        (v_copy, V_COPIES, v_send, v_pass),
    ):
        for i, entry in enumerate(table):
            a, g = entry[:2]
            copies[a, g].append(make(i, 0, 0, below(a, g), own_sem))
            if g == 2 or (g == 1 and a > 0):
                passed_on[a, g].append(make(i, a, g - 1, below(0, 1), pass_sem))

    def start(partner):
        for copy in copies[partner]:
            copy.start()

    by_block = sorted(PARTNERS, key=lambda partner: partner[1])
    for a, g in by_block:
        when(
            always(sends(a, g), jnp.logical_not(sends_over_end(a, g))),
            lambda a=a, g=g: start((a, g)),
        )
    for a, g in by_block:

        @pl.when(always(sends(a, g), sends_over_end(a, g)))
        def _():
            pl.semaphore_wait(ready.at[PARTNERS.index((a, g))], 1)
            start((a, g))

    def arrived(g):
        for a in range(3):
            if a or g:
                for copy in copies[a, g]:
                    copy.wait_recv()
        if g < 2:

            @pl.when(odd)
            def _():
                for a in range(3):
                    for copy in passed_on.get((a, g + 1), ()):
                        copy.start()

    def both_halves(a, g):
        value = load(edge, (a, g, 2), 2)
        store(tmp, (), value, 2, pl.ds(0, 4))
        store(tmp, (), value, 2, pl.ds(4, 4))
        return third_row(load(tmp, (), 2))

    def spread(matrix, rows, first):
        return per_element(lambda p: jnp.broadcast_to(p[first : first + 1], (8, 128)), matrix[:rows])

    def change_of_gauge(g):
        previous = None
        for a in (2, 1, 0):
            value = both_halves(a, 0)
            if g == 2:
                if a == 2:
                    value = matmul(value, both_halves(2, 1))
                else:
                    value = matmul(value, both_halves(a, 1))
            if a == 2:
                store(left, (2,), spread(value, 2, 0), 2)
                store(right, (2,), spread(value, 3, 1), 3)
            else:
                store(left, (a,), value[:2], 2)
                after = pick(time == 3, previous, rolled(value, 7))
                store(right, (a,), after, 3)
            previous = spread(value, 3, 0)

    def row_pair(a, g, piece, q):
        low = load(edge, (a, g, piece), 2, pl.ds(2 * q, 1))
        high = load(edge, (a, g, piece), 2, pl.ds(2 * q + 1, 1))
        wide = lambda p: jnp.broadcast_to(p, (8, 128))
        return third_row(per_element(lambda p, s: jnp.where(lower, wide(p), wide(s)), low, high))

    def into_window(value, a, g):
        if g > 0:
            value = third_row(matmul_dagger(value, load(right, (a,), 3)))
            value = matmul(load(left, (a,), 2), value)
        return third_row(value)

    def pair(g, q):
        xp = 2 * g + q
        for a in range(2):
            fix = pick(time == 3, row_pair(a + 1, g, 1, q), unit)
            value = matmul_dagger(load(field, (a, xp), 2), fix)
            store(tiles, (a,), into_window(value, a, g), 3)
        store(tiles, (2,), into_window(row_pair(2, g, 0, q)[:2], 2, g), 3)
        product = load(tiles, (0,), 3)
        store(chain, (0, xp), product, 3)
        for k in range(1, TMAX):
            if k < 4:
                here, after = load(tiles, (0,), 3), load(tiles, (1,), 3)
                factor = pick(time < 4 - k, rolled(here, -k), rolled(after, 4 - k))
            elif k == 4:
                factor = load(tiles, (1,), 3)
            else:
                factor = pick(time < 3, rolled(load(tiles, (1,), 3), -1), load(tiles, (2,), 3))
            product = third_row(matmul(product[:2], factor))
            store(chain, (k, xp), product, 3)

    lane = lax.broadcasted_iota(jnp.int32, (8, 128), 1)

    def correlate(sums, picked):
        def body(u, sums):
            totals = {}
            for c in range(18):
                tile = {}

                def even(m):
                    if m not in tile:
                        tile[m] = chain[u, m, c]
                    return tile[m]

                def turned(m):
                    if ("t", m) not in tile:
                        tile["t", m] = roll(even(m), 4)
                    return tile["t", m]

                def odd(m):
                    if ("o", m) not in tile:
                        tile["o", m] = jnp.where(lower, turned(m), turned(m + 1))
                    return tile["o", m]

                for r, xp in picked:
                    far = odd(xp + r // 2) if r % 2 else even(xp + r // 2)
                    term = even(xp) * far
                    totals[r, xp] = totals[r, xp] + term if (r, xp) in totals else term
            for r, xp in picked:
                total = jnp.sum(totals[r, xp], axis=1, keepdims=True)
                sums = jnp.where(lane == 8 * (2 * (r - 1) + xp) + u, total, sums)
            return sums

        return lax.fori_loop(0, TMAX, body, sums)

    def chains(g):
        def body(q, carry):
            pair(g, q)
            return carry

        lax.fori_loop(0, 2 if g < 2 else 1, body, 0)

    loops = [(r, xp) for r in range(1, RMAX + 1) for xp in range(2)]
    last = [(r, xp) for r, xp in loops if xp + (r + 1) // 2 == 4]
    arrived(0)
    change_of_gauge(1)
    chains(0)
    arrived(1)
    chains(1)
    change_of_gauge(2)
    sums = correlate(zero, [loop for loop in loops if loop not in last])
    arrived(2)
    chains(2)
    part[...] = correlate(sums, last)

    for a, g in PARTNERS:

        def sent(a=a, g=g):
            for copy in copies[a, g]:
                copy.wait_send()

        when(sends(a, g), sent)

    @pl.when(odd)
    def _():
        for partner in PARTNERS:
            for copy in passed_on[partner]:
                copy.wait_send()

    swap = pltpu.make_async_remote_copy(
        src_ref=part,
        dst_ref=peer,
        send_sem=sum_send,
        recv_sem=sum_recv,
        device_id={"gy": other_y},
        device_id_type=MESH,
    )

    @pl.when(y_at == 0)
    def _():
        pl.semaphore_wait(y_ready, 1)

    swap.start()
    swap.wait()
    sums = (part[...] + peer[...]) / (3.0 * 128 * n_y)
    for r, xp in loops:
        at = 8 * (2 * (r - 1) + xp)
        value = sums if at == 0 else pltpu.roll(sums, 128 - at, 1)
        out[r - 1, 2 * xp] = value[0:4, 0:TMAX]
        out[r - 1, 2 * xp + 1] = value[4:8, 0:TMAX]


def solution(mesh):
    sizes = tuple(mesh.shape[name] for name in ("gx", "gy", "ta"))

    def local(link_x, link_t):
        vmem = lambda *shape: pltpu.VMEM(shape, jnp.float32)
        sums = pl.pallas_call(
            lambda *refs: kernel(sizes, *refs),
            out_shape=jax.ShapeDtypeStruct((RMAX, 4, 4, TMAX), jnp.float32),
            in_specs=[pl.BlockSpec(memory_space=pl.ANY)] * 2,
            out_specs=pl.BlockSpec(memory_space=pltpu.VMEM),
            scratch_shapes=[
                vmem(18, 16, 128),
                vmem(18, 16, 128),
                vmem(2, 5, 12, 8, 128),
                vmem(3, 3, 3, 12, 4, 128),
                vmem(3, 12, 8, 128),
                vmem(3, 18, 8, 128),
                vmem(3, 18, 8, 128),
                vmem(TMAX, 5, 18, 8, 128),
                vmem(12, 8, 128),
                vmem(8, 128),
                vmem(8, 128),
                pltpu.SemaphoreType.DMA((2,)),
                pltpu.SemaphoreType.REGULAR((len(PARTNERS),)),
                pltpu.SemaphoreType.REGULAR,
                pltpu.SemaphoreType.DMA((len(V_COPIES),)),
                pltpu.SemaphoreType.DMA((len(V_COPIES),)),
                pltpu.SemaphoreType.DMA((len(V_COPIES),)),
                pltpu.SemaphoreType.DMA((len(E_COPIES),)),
                pltpu.SemaphoreType.DMA((len(E_COPIES),)),
                pltpu.SemaphoreType.DMA((len(E_COPIES),)),
                pltpu.SemaphoreType.DMA,
                pltpu.SemaphoreType.DMA,
            ],
            compiler_params=pltpu.CompilerParams(collective_id=0, has_side_effects=True),
        )(link_x.reshape(18, 16, 128), link_t.reshape(18, 16, 128))
        return sums.transpose(0, 3, 1, 2)

    return jax.shard_map(
        local,
        mesh=mesh,
        in_specs=(P(None, None, None, "gx", "ta", "gy"),) * 2,
        out_specs=P(None, None, "gx", "ta"),
        check_vma=False,
    )
```

```python
import jax
import jax.numpy as jnp
from jax import lax
from jax.experimental import pallas as pl
from jax.experimental.pallas import tpu as pltpu
from jax.sharding import PartitionSpec as P

RMAX = 6
TMAX = 6
MESH = pl.DeviceIdType.MESH

V_COPIES = ((1, 0, 2), (0, 1, 2), (1, 1, 2), (0, 2, 1), (1, 2, 1))
E_COPIES = (
    (1, 0, 1, 3),
    (2, 0, 0, 3),
    (0, 1, 2, 3),
    (1, 1, 1, 3),
    (2, 1, 0, 3),
    (1, 2, 1, 2),
    (2, 2, 0, 2),
)
PARTNERS = ((1, 0), (2, 0), (0, 1), (0, 2))


def cmul(a, b):
    return a[0] * b[0] - a[1] * b[1], a[0] * b[1] + a[1] * b[0]


def cmul_conj(a, b):
    return a[0] * b[0] + a[1] * b[1], a[1] * b[0] - a[0] * b[1]


def csum(terms):
    real, imag = terms[0]
    for term in terms[1:]:
        real, imag = real + term[0], imag + term[1]
    return real, imag


def matmul(a, b):
    return [[csum([cmul(row[j], b[j][k]) for j in range(3)]) for k in range(3)] for row in a]


def matmul_dagger(a, b):
    return [[csum([cmul_conj(row[j], b[k][j]) for j in range(3)]) for k in range(3)] for row in a]


def third_row(a):
    row = []
    for i in range(3):
        j, k = (i + 1) % 3, (i + 2) % 3
        first = cmul(a[0][j], a[1][k])
        second = cmul(a[0][k], a[1][j])
        row.append((first[0] - second[0], second[1] - first[1]))
    return [a[0], a[1], row]


def per_element(function, *matrices):
    return [
        [tuple(function(*(m[i][j][c] for m in matrices)) for c in range(2)) for j in range(3)]
        for i in range(len(matrices[0]))
    ]


def load(ref, lead, rows, window=slice(None)):
    return [
        [tuple(ref[(*lead, c * 3 * rows + i * 3 + j, window)] for c in range(2)) for j in range(3)]
        for i in range(rows)
    ]


def store(ref, lead, matrix, rows, window=slice(None)):
    for c in range(2):
        for i in range(rows):
            for j in range(3):
                ref[(*lead, c * 3 * rows + i * 3 + j, window)] = matrix[i][j][c]


def roll(value, shift):
    shift = shift % 8
    return value if shift == 0 else pltpu.roll(value, shift, 0)


def kernel(
    sizes, link_x, link_t, out, ux, ut, field, edge, left, right, tiles, chain, tmp, part, peer,
    in_sem, ready, y_ready, v_send, v_recv, v_next, v_second,
    e_send, e_recv, e_next, e_second, sum_send, sum_recv,
):
    n_x, n_y, n_t = sizes
    x_at, y_at, t_at = lax.axis_index("gx"), lax.axis_index("gy"), lax.axis_index("ta")
    other_y = lax.rem(y_at + 1, n_y)

    def above(a, g):
        return {"gx": lax.rem(x_at + g, n_x), "ta": lax.rem(t_at + a, n_t)}

    def below(a, g):
        return {"gx": lax.rem(x_at + n_x - g, n_x), "ta": lax.rem(t_at + n_t - a, n_t)}

    barrier = pltpu.get_barrier_semaphore()
    def always(*conditions):
        known = [c for c in conditions if isinstance(c, bool)]
        traced = [c for c in conditions if not isinstance(c, bool)]
        if not all(known):
            return False
        result = True
        for c in traced:
            result = c if result is True else result & c
        return result

    def when(condition, action):
        if condition is True:
            action()
        elif condition is not False:
            pl.when(condition)(action)

    odd = lax.rem(x_at, 2) == 1

    def sends(a, g):
        return odd if g == 2 else True

    def receives(a, g):
        return odd if g == 2 else True

    def sends_over_end(a, g):
        return (t_at < a) | (x_at < g)

    def receives_over_end(a, g):
        return (t_at + a >= n_t) | (x_at + g >= n_x)

    peers = (y_at > 0).astype(jnp.int32)
    for a, g in PARTNERS:

        @pl.when(always(receives(a, g), jnp.logical_not(receives_over_end(a, g))))
        def _():
            pl.semaphore_signal(barrier, inc=1, device_id=above(a, g), device_id_type=MESH)

        @pl.when(always(sends(a, g), sends_over_end(a, g)))
        def _():
            pl.semaphore_signal(barrier, inc=1, device_id=below(a, g), device_id_type=MESH)

        peers += always(sends(a, g), jnp.logical_not(sends_over_end(a, g))).astype(jnp.int32)
        peers += always(receives(a, g), receives_over_end(a, g)).astype(jnp.int32)

    @pl.when(y_at == 0)
    def _():
        pl.semaphore_signal(barrier, inc=1, device_id={"gy": other_y}, device_id_type=MESH)

    copy_x = pltpu.make_async_copy(link_x, ux, in_sem.at[0])
    copy_t = pltpu.make_async_copy(link_t, ut, in_sem.at[1])
    copy_x.start()
    copy_t.start()

    row = lax.broadcasted_iota(jnp.int32, (8, 128), 0)
    time = lax.rem(row, 4)
    lower = row < 4
    one = jnp.ones((8, 128), jnp.float32)
    zero = jnp.zeros((8, 128), jnp.float32)
    unit = [[(one if i == k else zero, zero) for k in range(3)] for i in range(3)]

    def pick(mask, a, b):
        return per_element(lambda p, q: jnp.where(mask, p, q), a, b)

    def rolled(a, shift):
        return per_element(lambda p: roll(p, shift), a)

    copy_x.wait()
    u0 = load(ux, (), 3, pl.ds(0, 8))
    u1 = load(ux, (), 3, pl.ds(8, 8))
    halves = matmul(pick(lower, u0, rolled(u1, 4)), pick(lower, rolled(u0, 4), u1))
    whole = matmul(pick(lower, halves, rolled(halves, 4)), pick(lower, u1, halves))
    starts = [
        pick(lower, unit, rolled(u0, 4)),
        pick(lower, halves, rolled(whole, 4)),
    ]
    store(edge, (0, 0, 2), per_element(lambda p: p[4:8], whole[:2]), 2)
    copy_t.wait()
    links = []
    for xp in range(2):
        begin = starts[xp]
        end = pick(time == 3, unit, rolled(begin, 7))
        v = matmul_dagger(matmul(begin[:2], load(ut, (), 3, pl.ds(8 * xp, 8))), end)
        store(field, (0, xp), v, 2)
        links.append(v)

    def first_times(low, high):
        value = jnp.where(row == 0, low, roll(low, -3))
        value = jnp.where(row == 2, roll(high, 2), value)
        return jnp.where(row == 3, roll(high, -1), value)[0:4]

    store(edge, (0, 0, 0), per_element(first_times, links[0], links[1]), 2)
    store(edge, (0, 0, 1), per_element(first_times, starts[0][:2], starts[1][:2]), 2)


    @pl.when(peers > 0)
    def _():
        pl.semaphore_wait(barrier, peers)

    for k, (a, g) in enumerate(PARTNERS):

        @pl.when(always(receives(a, g), receives_over_end(a, g)))
        def _():
            pl.semaphore_signal(ready.at[k], inc=1, device_id=above(a, g), device_id_type=MESH)

    @pl.when(y_at > 0)
    def _():
        pl.semaphore_signal(y_ready, inc=1, device_id={"gy": other_y}, device_id_type=MESH)

    def v_copy(i, a, g, target, send_sem):
        to_a, to_g, pairs = V_COPIES[i]
        return pltpu.make_async_remote_copy(
            src_ref=field.at[a, pl.ds(2 * g, pairs)],
            dst_ref=field.at[to_a, pl.ds(2 * to_g, pairs)],
            send_sem=send_sem.at[i],
            recv_sem=v_recv.at[i],
            device_id=target,
            device_id_type=MESH,
        )

    def e_copy(i, a, g, target, send_sem):
        to_a, to_g, first, last = E_COPIES[i]
        return pltpu.make_async_remote_copy(
            src_ref=edge.at[a, g, pl.ds(first, last - first)],
            dst_ref=edge.at[to_a, to_g, pl.ds(first, last - first)],
            send_sem=send_sem.at[i],
            recv_sem=e_recv.at[i],
            device_id=target,
            device_id_type=MESH,
        )

    slots = [(a, g) for g in range(3) for a in range(3) if a or g]
    copies = {slot: [] for slot in slots}
    to_next = {slot: [] for slot in slots}
    to_second = {slot: [] for slot in slots}
    for make, table, own_sem, next_sem, second_sem in (
        (e_copy, E_COPIES, e_send, e_next, e_second),
        (v_copy, V_COPIES, v_send, v_next, v_second),
    ):
        for i, entry in enumerate(table):
            a, g = entry[:2]
            copies[a, g].append(make(i, 0, 0, below(a, g), own_sem))
            if g == 2 or (g == 1 and a > 0):
                to_next[a, g - 1].append(make(i, a, g - 1, below(0, 1), next_sem))
            if g == 2 and a > 0:
                to_second[a, 0].append(make(i, a, 0, below(0, 2), second_sem))

    def start(partner):
        for copy in copies[partner]:
            copy.start()

    for a, g in PARTNERS:
        when(
            always(sends(a, g), jnp.logical_not(sends_over_end(a, g))),
            lambda a=a, g=g: start((a, g)),
        )
    for a, g in PARTNERS:

        @pl.when(always(sends(a, g), sends_over_end(a, g)))
        def _():
            pl.semaphore_wait(ready.at[PARTNERS.index((a, g))], 1)
            start((a, g))

    def each(some):
        def start_all():
            for copy in some:
                copy.start()

        return start_all

    def arrived(g):
        for a, slot_g in slots:
            if slot_g == g:
                for copy in copies[a, g]:
                    copy.wait_recv()
                onward = to_next[a, g]
                when(odd if g == 1 else bool(onward), each(onward))
                if to_second[a, g]:
                    when(odd, each(to_second[a, g]))

    def both_halves(a, g):
        value = load(edge, (a, g, 2), 2)
        store(tmp, (), value, 2, pl.ds(0, 4))
        store(tmp, (), value, 2, pl.ds(4, 4))
        return third_row(load(tmp, (), 2))

    def spread(matrix, rows, first):
        return per_element(lambda p: jnp.broadcast_to(p[first : first + 1], (8, 128)), matrix[:rows])

    def change_of_gauge(g):
        previous = None
        for a in (2, 1, 0):
            value = both_halves(a, 0)
            if g == 2:
                if a == 2:
                    value = matmul(value, both_halves(2, 1))
                else:
                    value = matmul(value, both_halves(a, 1))
            if a == 2:
                store(left, (2,), spread(value, 2, 0), 2)
                store(right, (2,), spread(value, 3, 1), 3)
            else:
                store(left, (a,), value[:2], 2)
                after = pick(time == 3, previous, rolled(value, 7))
                store(right, (a,), after, 3)
            previous = spread(value, 3, 0)

    def row_pair(a, g, piece, q):
        low = load(edge, (a, g, piece), 2, pl.ds(2 * q, 1))
        high = load(edge, (a, g, piece), 2, pl.ds(2 * q + 1, 1))
        wide = lambda p: jnp.broadcast_to(p, (8, 128))
        return third_row(per_element(lambda p, s: jnp.where(lower, wide(p), wide(s)), low, high))

    def into_window(value, a, g):
        if g > 0:
            value = third_row(matmul_dagger(value, load(right, (a,), 3)))
            value = matmul(load(left, (a,), 2), value)
        return third_row(value)

    def pair(g, q):
        xp = 2 * g + q
        for a in range(2):
            fix = pick(time == 3, row_pair(a + 1, g, 1, q), unit)
            value = matmul_dagger(load(field, (a, xp), 2), fix)
            store(tiles, (a,), into_window(value, a, g), 3)
        store(tiles, (2,), into_window(row_pair(2, g, 0, q)[:2], 2, g), 3)
        product = load(tiles, (0,), 3)
        store(chain, (0, xp), product, 3)
        for k in range(1, TMAX):
            if k < 4:
                here, after = load(tiles, (0,), 3), load(tiles, (1,), 3)
                factor = pick(time < 4 - k, rolled(here, -k), rolled(after, 4 - k))
            elif k == 4:
                factor = load(tiles, (1,), 3)
            else:
                factor = pick(time < 3, rolled(load(tiles, (1,), 3), -1), load(tiles, (2,), 3))
            product = third_row(matmul(product[:2], factor))
            store(chain, (k, xp), product, 3)

    lane = lax.broadcasted_iota(jnp.int32, (8, 128), 1)

    def correlate(sums, picked):
        def body(u, sums):
            totals = {}
            for c in range(18):
                tile = {}

                def even(m):
                    if m not in tile:
                        tile[m] = chain[u, m, c]
                    return tile[m]

                def turned(m):
                    if ("t", m) not in tile:
                        tile["t", m] = roll(even(m), 4)
                    return tile["t", m]

                def odd(m):
                    if ("o", m) not in tile:
                        tile["o", m] = jnp.where(lower, turned(m), turned(m + 1))
                    return tile["o", m]

                for r, xp in picked:
                    far = odd(xp + r // 2) if r % 2 else even(xp + r // 2)
                    term = even(xp) * far
                    totals[r, xp] = totals[r, xp] + term if (r, xp) in totals else term
            for r, xp in picked:
                total = jnp.sum(totals[r, xp], axis=1, keepdims=True)
                sums = jnp.where(lane == 8 * (2 * (r - 1) + xp) + u, total, sums)
            return sums

        return lax.fori_loop(0, TMAX, body, sums)

    def chains(g):
        def body(q, carry):
            pair(g, q)
            return carry

        lax.fori_loop(0, 2 if g < 2 else 1, body, 0)

    loops = [(r, xp) for r in range(1, RMAX + 1) for xp in range(2)]
    last = [(r, xp) for r, xp in loops if xp + (r + 1) // 2 == 4]
    arrived(0)
    change_of_gauge(1)
    chains(0)
    arrived(1)
    chains(1)
    change_of_gauge(2)
    sums = correlate(zero, [loop for loop in loops if loop not in last])
    arrived(2)
    chains(2)
    part[...] = correlate(sums, last)

    for a, g in PARTNERS:

        def sent(a=a, g=g):
            for copy in copies[a, g]:
                copy.wait_send()

        when(sends(a, g), sent)

    for slot in slots:

        def relayed(some):
            def wait_all():
                for copy in some:
                    copy.wait_send()

            return wait_all

        if to_next[slot]:
            when(odd if slot[1] == 1 else True, relayed(to_next[slot]))
        if to_second[slot]:
            when(odd, relayed(to_second[slot]))

    swap = pltpu.make_async_remote_copy(
        src_ref=part,
        dst_ref=peer,
        send_sem=sum_send,
        recv_sem=sum_recv,
        device_id={"gy": other_y},
        device_id_type=MESH,
    )

    @pl.when(y_at == 0)
    def _():
        pl.semaphore_wait(y_ready, 1)

    swap.start()
    swap.wait()
    sums = (part[...] + peer[...]) / (3.0 * 128 * n_y)
    for r, xp in loops:
        at = 8 * (2 * (r - 1) + xp)
        value = sums if at == 0 else pltpu.roll(sums, 128 - at, 1)
        out[r - 1, 2 * xp] = value[0:4, 0:TMAX]
        out[r - 1, 2 * xp + 1] = value[4:8, 0:TMAX]


def solution(mesh):
    sizes = tuple(mesh.shape[name] for name in ("gx", "gy", "ta"))

    def local(link_x, link_t):
        vmem = lambda *shape: pltpu.VMEM(shape, jnp.float32)
        sums = pl.pallas_call(
            lambda *refs: kernel(sizes, *refs),
            out_shape=jax.ShapeDtypeStruct((RMAX, 4, 4, TMAX), jnp.float32),
            in_specs=[pl.BlockSpec(memory_space=pl.ANY)] * 2,
            out_specs=pl.BlockSpec(memory_space=pltpu.VMEM),
            scratch_shapes=[
                vmem(18, 16, 128),
                vmem(18, 16, 128),
                vmem(2, 5, 12, 8, 128),
                vmem(3, 3, 3, 12, 4, 128),
                vmem(3, 12, 8, 128),
                vmem(3, 18, 8, 128),
                vmem(3, 18, 8, 128),
                vmem(TMAX, 5, 18, 8, 128),
                vmem(12, 8, 128),
                vmem(8, 128),
                vmem(8, 128),
                pltpu.SemaphoreType.DMA((2,)),
                pltpu.SemaphoreType.REGULAR((len(PARTNERS),)),
                pltpu.SemaphoreType.REGULAR,
                pltpu.SemaphoreType.DMA((len(V_COPIES),)),
                pltpu.SemaphoreType.DMA((len(V_COPIES),)),
                pltpu.SemaphoreType.DMA((len(V_COPIES),)),
                pltpu.SemaphoreType.DMA((len(V_COPIES),)),
                pltpu.SemaphoreType.DMA((len(E_COPIES),)),
                pltpu.SemaphoreType.DMA((len(E_COPIES),)),
                pltpu.SemaphoreType.DMA((len(E_COPIES),)),
                pltpu.SemaphoreType.DMA((len(E_COPIES),)),
                pltpu.SemaphoreType.DMA,
                pltpu.SemaphoreType.DMA,
            ],
            compiler_params=pltpu.CompilerParams(collective_id=0, has_side_effects=True),
        )(link_x.reshape(18, 16, 128), link_t.reshape(18, 16, 128))
        return sums.transpose(0, 3, 1, 2)

    return jax.shard_map(
        local,
        mesh=mesh,
        in_specs=(P(None, None, None, "gx", "ta", "gy"),) * 2,
        out_specs=P(None, None, "gx", "ta"),
        check_vma=False,
    )
```

```python
import jax
import jax.numpy as jnp
from jax import lax
from jax.experimental import pallas as pl
from jax.experimental.pallas import tpu as pltpu
from jax.sharding import PartitionSpec as P

RMAX = 6
TMAX = 6
MESH = pl.DeviceIdType.MESH

V_COPIES = ((1, 0, 0), (1, 0, 1), (0, 1, 0), (0, 1, 1), (1, 1, 0), (1, 1, 1), (0, 2, 0), (1, 2, 0))
E_COPIES = (
    (1, 0, 1, 3),
    (2, 0, 0, 3),
    (0, 1, 2, 3),
    (1, 1, 1, 3),
    (2, 1, 0, 3),
    (1, 2, 1, 2),
    (2, 2, 0, 2),
)
PARTNERS = ((0, 1), (0, 2), (1, 0), (2, 0))
ORDER = (
    ("E", 1, 0),
    ("E", 2, 0),
    ("V", 0, 1, 0),
    ("V", 1, 0, 0),
    ("V", 0, 2, 0),
    ("V", 1, 0, 1),
    ("V", 0, 1, 1),
    ("E", 0, 1),
)


def cmul(a, b):
    return a[0] * b[0] - a[1] * b[1], a[0] * b[1] + a[1] * b[0]


def cmul_conj(a, b):
    return a[0] * b[0] + a[1] * b[1], a[1] * b[0] - a[0] * b[1]


def csum(terms):
    real, imag = terms[0]
    for term in terms[1:]:
        real, imag = real + term[0], imag + term[1]
    return real, imag


def matmul(a, b):
    return [[csum([cmul(row[j], b[j][k]) for j in range(3)]) for k in range(3)] for row in a]


def matmul_dagger(a, b):
    return [[csum([cmul_conj(row[j], b[k][j]) for j in range(3)]) for k in range(3)] for row in a]


def third_row(a):
    row = []
    for i in range(3):
        j, k = (i + 1) % 3, (i + 2) % 3
        first = cmul(a[0][j], a[1][k])
        second = cmul(a[0][k], a[1][j])
        row.append((first[0] - second[0], second[1] - first[1]))
    return [a[0], a[1], row]


def per_element(function, *matrices):
    return [
        [tuple(function(*(m[i][j][c] for m in matrices)) for c in range(2)) for j in range(3)]
        for i in range(len(matrices[0]))
    ]


def load(ref, lead, rows, window=slice(None)):
    return [
        [tuple(ref[(*lead, c * 3 * rows + i * 3 + j, window)] for c in range(2)) for j in range(3)]
        for i in range(rows)
    ]


def store(ref, lead, matrix, rows, window=slice(None)):
    for c in range(2):
        for i in range(rows):
            for j in range(3):
                ref[(*lead, c * 3 * rows + i * 3 + j, window)] = matrix[i][j][c]


def roll(value, shift):
    shift = shift % 8
    return value if shift == 0 else pltpu.roll(value, shift, 0)


def kernel(
    sizes, link_x, link_t, out, ux, ut, field, edge, left, right, tiles, chain, tmp, part, peer,
    in_sem, ready, y_ready, v_send, v_recv, v_next, v_second,
    e_send, e_recv, e_next, e_second, sum_send, sum_recv,
):
    n_x, n_y, n_t = sizes
    x_at, y_at, t_at = lax.axis_index("gx"), lax.axis_index("gy"), lax.axis_index("ta")
    other_y = lax.rem(y_at + 1, n_y)

    def above(a, g):
        return {"gx": lax.rem(x_at + g, n_x), "ta": lax.rem(t_at + a, n_t)}

    def below(a, g):
        return {"gx": lax.rem(x_at + n_x - g, n_x), "ta": lax.rem(t_at + n_t - a, n_t)}

    barrier = pltpu.get_barrier_semaphore()
    def always(*conditions):
        known = [c for c in conditions if isinstance(c, bool)]
        traced = [c for c in conditions if not isinstance(c, bool)]
        if not all(known):
            return False
        result = True
        for c in traced:
            result = c if result is True else result & c
        return result

    def when(condition, action):
        if condition is True:
            action()
        elif condition is not False:
            pl.when(condition)(action)

    odd = lax.rem(x_at, 2) == 1

    def sends(a, g):
        return odd if g == 2 else True

    def receives(a, g):
        return odd if g == 2 else True

    def sends_over_end(a, g):
        return (t_at < a) | (x_at < g)

    def receives_over_end(a, g):
        return (t_at + a >= n_t) | (x_at + g >= n_x)

    peers = (y_at > 0).astype(jnp.int32)
    for a, g in PARTNERS:

        @pl.when(always(receives(a, g), jnp.logical_not(receives_over_end(a, g))))
        def _():
            pl.semaphore_signal(barrier, inc=1, device_id=above(a, g), device_id_type=MESH)

        @pl.when(always(sends(a, g), sends_over_end(a, g)))
        def _():
            pl.semaphore_signal(barrier, inc=1, device_id=below(a, g), device_id_type=MESH)

        peers += always(sends(a, g), jnp.logical_not(sends_over_end(a, g))).astype(jnp.int32)
        peers += always(receives(a, g), receives_over_end(a, g)).astype(jnp.int32)

    @pl.when(y_at == 0)
    def _():
        pl.semaphore_signal(barrier, inc=1, device_id={"gy": other_y}, device_id_type=MESH)

    copy_x = pltpu.make_async_copy(link_x, ux, in_sem.at[0])
    copy_t = pltpu.make_async_copy(link_t, ut, in_sem.at[1])
    copy_x.start()
    copy_t.start()

    row = lax.broadcasted_iota(jnp.int32, (8, 128), 0)
    time = lax.rem(row, 4)
    lower = row < 4
    one = jnp.ones((8, 128), jnp.float32)
    zero = jnp.zeros((8, 128), jnp.float32)
    unit = [[(one if i == k else zero, zero) for k in range(3)] for i in range(3)]

    def pick(mask, a, b):
        return per_element(lambda p, q: jnp.where(mask, p, q), a, b)

    def rolled(a, shift):
        return per_element(lambda p: roll(p, shift), a)

    copy_x.wait()
    u0 = load(ux, (), 3, pl.ds(0, 8))
    u1 = load(ux, (), 3, pl.ds(8, 8))
    halves = matmul(pick(lower, u0, rolled(u1, 4)), pick(lower, rolled(u0, 4), u1))
    whole = matmul(pick(lower, halves, rolled(halves, 4)), pick(lower, u1, halves))
    starts = [
        pick(lower, unit, rolled(u0, 4)),
        pick(lower, halves, rolled(whole, 4)),
    ]
    store(edge, (0, 0, 2), per_element(lambda p: p[4:8], whole[:2]), 2)
    copy_t.wait()
    links = []
    for xp in range(2):
        begin = starts[xp]
        end = pick(time == 3, unit, rolled(begin, 7))
        v = matmul_dagger(matmul(begin[:2], load(ut, (), 3, pl.ds(8 * xp, 8))), end)
        store(field, (0, xp), v, 2)
        links.append(v)

    def first_times(low, high):
        value = jnp.where(row == 0, low, roll(low, -3))
        value = jnp.where(row == 2, roll(high, 2), value)
        return jnp.where(row == 3, roll(high, -1), value)[0:4]

    store(edge, (0, 0, 0), per_element(first_times, links[0], links[1]), 2)
    store(edge, (0, 0, 1), per_element(first_times, starts[0][:2], starts[1][:2]), 2)


    @pl.when(peers > 0)
    def _():
        pl.semaphore_wait(barrier, peers)

    for k, (a, g) in enumerate(PARTNERS):

        @pl.when(always(receives(a, g), receives_over_end(a, g)))
        def _():
            pl.semaphore_signal(ready.at[k], inc=1, device_id=above(a, g), device_id_type=MESH)

    @pl.when(y_at > 0)
    def _():
        pl.semaphore_signal(y_ready, inc=1, device_id={"gy": other_y}, device_id_type=MESH)

    def v_copy(i, a, g, target, send_sem):
        to_a, to_g, pair = V_COPIES[i]
        return pltpu.make_async_remote_copy(
            src_ref=field.at[a, 2 * g + pair],
            dst_ref=field.at[to_a, 2 * to_g + pair],
            send_sem=send_sem.at[i],
            recv_sem=v_recv.at[i],
            device_id=target,
            device_id_type=MESH,
        )

    def e_copy(i, a, g, target, send_sem):
        to_a, to_g, first, last = E_COPIES[i]
        return pltpu.make_async_remote_copy(
            src_ref=edge.at[a, g, pl.ds(first, last - first)],
            dst_ref=edge.at[to_a, to_g, pl.ds(first, last - first)],
            send_sem=send_sem.at[i],
            recv_sem=e_recv.at[i],
            device_id=target,
            device_id_type=MESH,
        )

    copies, to_next, to_second = {}, {}, {}
    for name, make, table, own_sem, next_sem, second_sem in (
        ("E", e_copy, E_COPIES, e_send, e_next, e_second),
        ("V", v_copy, V_COPIES, v_send, v_next, v_second),
    ):
        for i, entry in enumerate(table):
            a, g = entry[:2]
            tile = entry[2:] if name == "V" else ()
            copies[(name, a, g, *tile)] = make(i, 0, 0, below(a, g), own_sem)
            if g == 2 or (g == 1 and a > 0):
                to_next[(name, a, g - 1, *tile)] = make(i, a, g - 1, below(0, 1), next_sem)
            if g == 2 and a > 0:
                to_second[(name, a, 0, *tile)] = make(i, a, 0, below(0, 2), second_sem)

    def start(*partners):
        for key in ORDER:
            if key[1:3] in partners:
                copies[key].start()

    for key in ORDER:
        a, g = key[1:3]
        when(always(sends(a, g), jnp.logical_not(sends_over_end(a, g))), copies[key].start)

    def send_over_end(*partners):
        for a, g in partners:

            @pl.when(always(sends(a, g), sends_over_end(a, g)))
            def _():
                pl.semaphore_wait(ready.at[PARTNERS.index((a, g))], 1)
                start((a, g))

    def take(*keys):
        for key in keys:
            copies[key].wait_recv()
            if key in to_next:
                when(odd if key[2] == 1 else True, to_next[key].start)
            if key in to_second:
                when(odd, to_second[key].start)

    def both_halves(a, g):
        value = load(edge, (a, g, 2), 2)
        store(tmp, (), value, 2, pl.ds(0, 4))
        store(tmp, (), value, 2, pl.ds(4, 4))
        return third_row(load(tmp, (), 2))

    def spread(matrix, rows, first):
        return per_element(lambda p: jnp.broadcast_to(p[first : first + 1], (8, 128)), matrix[:rows])

    def change_of_gauge(g):
        previous = None
        for a in (2, 1, 0):
            value = both_halves(a, 0)
            if g == 2:
                if a == 2:
                    value = matmul(value, both_halves(2, 1))
                else:
                    value = matmul(value, both_halves(a, 1))
            if a == 2:
                store(left, (2,), spread(value, 2, 0), 2)
                store(right, (2,), spread(value, 3, 1), 3)
            else:
                store(left, (a,), value[:2], 2)
                after = pick(time == 3, previous, rolled(value, 7))
                store(right, (a,), after, 3)
            previous = spread(value, 3, 0)

    def row_pair(a, g, piece, q):
        low = load(edge, (a, g, piece), 2, pl.ds(2 * q, 1))
        high = load(edge, (a, g, piece), 2, pl.ds(2 * q + 1, 1))
        wide = lambda p: jnp.broadcast_to(p, (8, 128))
        return third_row(per_element(lambda p, s: jnp.where(lower, wide(p), wide(s)), low, high))

    def into_window(value, a, g):
        if g > 0:
            value = third_row(matmul_dagger(value, load(right, (a,), 3)))
            value = matmul(load(left, (a,), 2), value)
        return third_row(value)

    def pair(g, q):
        xp = 2 * g + q
        for a in range(2):
            fix = pick(time == 3, row_pair(a + 1, g, 1, q), unit)
            value = matmul_dagger(load(field, (a, xp), 2), fix)
            store(tiles, (a,), into_window(value, a, g), 3)
        store(tiles, (2,), into_window(row_pair(2, g, 0, q)[:2], 2, g), 3)
        product = load(tiles, (0,), 3)
        store(chain, (0, xp), product, 3)
        for k in range(1, TMAX):
            if k < 4:
                here, after = load(tiles, (0,), 3), load(tiles, (1,), 3)
                factor = pick(time < 4 - k, rolled(here, -k), rolled(after, 4 - k))
            elif k == 4:
                factor = load(tiles, (1,), 3)
            else:
                factor = pick(time < 3, rolled(load(tiles, (1,), 3), -1), load(tiles, (2,), 3))
            product = third_row(matmul(product[:2], factor))
            store(chain, (k, xp), product, 3)

    lane = lax.broadcasted_iota(jnp.int32, (8, 128), 1)

    def correlate(sums, picked):
        def body(u, sums):
            totals = {}
            for c in range(18):
                tile = {}

                def even(m):
                    if m not in tile:
                        tile[m] = chain[u, m, c]
                    return tile[m]

                def turned(m):
                    if ("t", m) not in tile:
                        tile["t", m] = roll(even(m), 4)
                    return tile["t", m]

                def odd(m):
                    if ("o", m) not in tile:
                        tile["o", m] = jnp.where(lower, turned(m), turned(m + 1))
                    return tile["o", m]

                for r, xp in picked:
                    far = odd(xp + r // 2) if r % 2 else even(xp + r // 2)
                    term = even(xp) * far
                    totals[r, xp] = totals[r, xp] + term if (r, xp) in totals else term
            for r, xp in picked:
                total = jnp.sum(totals[r, xp], axis=1, keepdims=True)
                sums = jnp.where(lane == 8 * (2 * (r - 1) + xp) + u, total, sums)
            return sums

        return lax.fori_loop(0, TMAX, body, sums)

    def chains(g):
        def body(q, carry):
            pair(g, q)
            return carry

        lax.fori_loop(0, 2 if g < 2 else 1, body, 0)

    loops = [(r, xp) for r in range(1, RMAX + 1) for xp in range(2)]
    last = [(r, xp) for r, xp in loops if xp + (r + 1) // 2 == 4]
    send_over_end((0, 1), (0, 2))
    take(("V", 0, 1, 0), ("E", 1, 0), ("E", 2, 0))
    send_over_end((1, 0), (2, 0))
    take(("V", 1, 0, 0), ("E", 1, 1), ("E", 2, 1), ("V", 1, 0, 1))
    change_of_gauge(1)
    chains(0)
    take(("V", 1, 1, 0), ("V", 0, 1, 1), ("E", 0, 1), ("V", 1, 1, 1))
    chains(1)
    change_of_gauge(2)
    sums = correlate(zero, [loop for loop in loops if loop not in last])
    take(("E", 1, 2), ("E", 2, 2), ("V", 0, 2, 0), ("V", 1, 2, 0))
    chains(2)
    part[...] = correlate(sums, last)

    for key in ORDER:
        when(sends(*key[1:3]), copies[key].wait_send)
    for key, copy in to_next.items():
        when(odd if key[2] == 1 else True, copy.wait_send)
    for copy in to_second.values():
        when(odd, copy.wait_send)
    swap = pltpu.make_async_remote_copy(
        src_ref=part,
        dst_ref=peer,
        send_sem=sum_send,
        recv_sem=sum_recv,
        device_id={"gy": other_y},
        device_id_type=MESH,
    )

    @pl.when(y_at == 0)
    def _():
        pl.semaphore_wait(y_ready, 1)

    swap.start()
    swap.wait()
    sums = (part[...] + peer[...]) / (3.0 * 128 * n_y)
    for r, xp in loops:
        at = 8 * (2 * (r - 1) + xp)
        value = sums if at == 0 else pltpu.roll(sums, 128 - at, 1)
        out[r - 1, 2 * xp] = value[0:4, 0:TMAX]
        out[r - 1, 2 * xp + 1] = value[4:8, 0:TMAX]


def solution(mesh):
    sizes = tuple(mesh.shape[name] for name in ("gx", "gy", "ta"))

    def local(link_x, link_t):
        vmem = lambda *shape: pltpu.VMEM(shape, jnp.float32)
        sums = pl.pallas_call(
            lambda *refs: kernel(sizes, *refs),
            out_shape=jax.ShapeDtypeStruct((RMAX, 4, 4, TMAX), jnp.float32),
            in_specs=[pl.BlockSpec(memory_space=pl.ANY)] * 2,
            out_specs=pl.BlockSpec(memory_space=pltpu.VMEM),
            scratch_shapes=[
                vmem(18, 16, 128),
                vmem(18, 16, 128),
                vmem(2, 5, 12, 8, 128),
                vmem(3, 3, 3, 12, 4, 128),
                vmem(3, 12, 8, 128),
                vmem(3, 18, 8, 128),
                vmem(3, 18, 8, 128),
                vmem(TMAX, 5, 18, 8, 128),
                vmem(12, 8, 128),
                vmem(8, 128),
                vmem(8, 128),
                pltpu.SemaphoreType.DMA((2,)),
                pltpu.SemaphoreType.REGULAR((len(PARTNERS),)),
                pltpu.SemaphoreType.REGULAR,
                pltpu.SemaphoreType.DMA((len(V_COPIES),)),
                pltpu.SemaphoreType.DMA((len(V_COPIES),)),
                pltpu.SemaphoreType.DMA((len(V_COPIES),)),
                pltpu.SemaphoreType.DMA((len(V_COPIES),)),
                pltpu.SemaphoreType.DMA((len(E_COPIES),)),
                pltpu.SemaphoreType.DMA((len(E_COPIES),)),
                pltpu.SemaphoreType.DMA((len(E_COPIES),)),
                pltpu.SemaphoreType.DMA((len(E_COPIES),)),
                pltpu.SemaphoreType.DMA,
                pltpu.SemaphoreType.DMA,
            ],
            compiler_params=pltpu.CompilerParams(collective_id=0, has_side_effects=True),
        )(link_x.reshape(18, 16, 128), link_t.reshape(18, 16, 128))
        return sums.transpose(0, 3, 1, 2)

    return jax.shard_map(
        local,
        mesh=mesh,
        in_specs=(P(None, None, None, "gx", "ta", "gy"),) * 2,
        out_specs=P(None, None, "gx", "ta"),
        check_vma=False,
    )
```

```python
import jax
import jax.numpy as jnp
from jax import lax
from jax.experimental import pallas as pl
from jax.experimental.pallas import tpu as pltpu
from jax.sharding import PartitionSpec as P

RMAX = 6
TMAX = 6
MESH = pl.DeviceIdType.MESH

V_COPIES = ((1, 0, 2), (0, 1, 2), (1, 1, 2), (0, 2, 1), (1, 2, 1))
E_COPIES = (
    (1, 0, 1, 3),
    (2, 0, 0, 3),
    (0, 1, 2, 3),
    (1, 1, 1, 3),
    (2, 1, 0, 3),
    (1, 2, 1, 2),
    (2, 2, 0, 2),
)
PARTNERS = ((1, 0), (2, 0), (0, 1), (0, 2))


def cmul(a, b):
    return a[0] * b[0] - a[1] * b[1], a[0] * b[1] + a[1] * b[0]


def cmul_conj(a, b):
    return a[0] * b[0] + a[1] * b[1], a[1] * b[0] - a[0] * b[1]


def csum(terms):
    real, imag = terms[0]
    for term in terms[1:]:
        real, imag = real + term[0], imag + term[1]
    return real, imag


def matmul(a, b):
    return [[csum([cmul(row[j], b[j][k]) for j in range(3)]) for k in range(3)] for row in a]


def matmul_dagger(a, b):
    return [[csum([cmul_conj(row[j], b[k][j]) for j in range(3)]) for k in range(3)] for row in a]


def third_row(a):
    row = []
    for i in range(3):
        j, k = (i + 1) % 3, (i + 2) % 3
        first = cmul(a[0][j], a[1][k])
        second = cmul(a[0][k], a[1][j])
        row.append((first[0] - second[0], second[1] - first[1]))
    return [a[0], a[1], row]


def per_element(function, *matrices):
    return [
        [tuple(function(*(m[i][j][c] for m in matrices)) for c in range(2)) for j in range(3)]
        for i in range(len(matrices[0]))
    ]


def load(ref, lead, rows, window=slice(None)):
    return [
        [tuple(ref[(*lead, c * 3 * rows + i * 3 + j, window)] for c in range(2)) for j in range(3)]
        for i in range(rows)
    ]


def store(ref, lead, matrix, rows, window=slice(None)):
    for c in range(2):
        for i in range(rows):
            for j in range(3):
                ref[(*lead, c * 3 * rows + i * 3 + j, window)] = matrix[i][j][c]


def roll(value, shift):
    shift = shift % 8
    return value if shift == 0 else pltpu.roll(value, shift, 0)


def kernel(
    sizes, link_x, link_t, out, ux, ut, field, edge, left, right, tiles, chain, tmp, part, peer,
    in_sem, ready, y_ready, v_send, v_recv, v_next, v_second,
    e_send, e_recv, e_next, e_second, sum_send, sum_recv,
):
    n_x, n_y, n_t = sizes
    x_at, y_at, t_at = lax.axis_index("gx"), lax.axis_index("gy"), lax.axis_index("ta")
    other_y = lax.rem(y_at + 1, n_y)

    def above(a, g):
        return {"gx": lax.rem(x_at + g, n_x), "ta": lax.rem(t_at + a, n_t)}

    def below(a, g):
        return {"gx": lax.rem(x_at + n_x - g, n_x), "ta": lax.rem(t_at + n_t - a, n_t)}

    barrier = pltpu.get_barrier_semaphore()
    def always(*conditions):
        known = [c for c in conditions if isinstance(c, bool)]
        traced = [c for c in conditions if not isinstance(c, bool)]
        if not all(known):
            return False
        result = True
        for c in traced:
            result = c if result is True else result & c
        return result

    def when(condition, action):
        if condition is True:
            action()
        elif condition is not False:
            pl.when(condition)(action)

    odd = lax.rem(x_at, 2) == 1

    def sends(a, g):
        return odd if g == 2 else True

    def receives(a, g):
        return odd if g == 2 else True

    def sends_over_end(a, g):
        return (t_at < a) | (x_at < g)

    def receives_over_end(a, g):
        return (t_at + a >= n_t) | (x_at + g >= n_x)

    peers = (y_at > 0).astype(jnp.int32)
    for a, g in PARTNERS:

        @pl.when(always(receives(a, g), jnp.logical_not(receives_over_end(a, g))))
        def _():
            pl.semaphore_signal(barrier, inc=1, device_id=above(a, g), device_id_type=MESH)

        @pl.when(always(sends(a, g), sends_over_end(a, g)))
        def _():
            pl.semaphore_signal(barrier, inc=1, device_id=below(a, g), device_id_type=MESH)

        peers += always(sends(a, g), jnp.logical_not(sends_over_end(a, g))).astype(jnp.int32)
        peers += always(receives(a, g), receives_over_end(a, g)).astype(jnp.int32)

    @pl.when(y_at == 0)
    def _():
        pl.semaphore_signal(barrier, inc=1, device_id={"gy": other_y}, device_id_type=MESH)

    copy_x = pltpu.make_async_copy(link_x, ux, in_sem.at[0])
    copy_t = pltpu.make_async_copy(link_t, ut, in_sem.at[1])
    copy_x.start()
    copy_t.start()

    row = lax.broadcasted_iota(jnp.int32, (8, 128), 0)
    time = lax.rem(row, 4)
    lower = row < 4
    one = jnp.ones((8, 128), jnp.float32)
    zero = jnp.zeros((8, 128), jnp.float32)
    unit = [[(one if i == k else zero, zero) for k in range(3)] for i in range(3)]

    def pick(mask, a, b):
        return per_element(lambda p, q: jnp.where(mask, p, q), a, b)

    def rolled(a, shift):
        return per_element(lambda p: roll(p, shift), a)

    copy_x.wait()
    u0 = load(ux, (), 3, pl.ds(0, 8))
    u1 = load(ux, (), 3, pl.ds(8, 8))
    halves = matmul(pick(lower, u0, rolled(u1, 4)), pick(lower, rolled(u0, 4), u1))
    whole = matmul(pick(lower, halves, rolled(halves, 4)), pick(lower, u1, halves))
    starts = [
        pick(lower, unit, rolled(u0, 4)),
        pick(lower, halves, rolled(whole, 4)),
    ]
    store(edge, (0, 0, 2), per_element(lambda p: p[4:8], whole[:2]), 2)
    copy_t.wait()
    links = []
    for xp in range(2):
        begin = starts[xp]
        end = pick(time == 3, unit, rolled(begin, 7))
        v = matmul_dagger(matmul(begin[:2], load(ut, (), 3, pl.ds(8 * xp, 8))), end)
        store(field, (0, xp), v, 2)
        links.append(v)

    def first_times(low, high):
        value = jnp.where(row == 0, low, roll(low, -3))
        value = jnp.where(row == 2, roll(high, 2), value)
        return jnp.where(row == 3, roll(high, -1), value)[0:4]

    store(edge, (0, 0, 0), per_element(first_times, links[0], links[1]), 2)
    store(edge, (0, 0, 1), per_element(first_times, starts[0][:2], starts[1][:2]), 2)


    @pl.when(peers > 0)
    def _():
        pl.semaphore_wait(barrier, peers)

    for k, (a, g) in enumerate(PARTNERS):

        @pl.when(always(receives(a, g), receives_over_end(a, g)))
        def _():
            pl.semaphore_signal(ready.at[k], inc=1, device_id=above(a, g), device_id_type=MESH)

    @pl.when(y_at > 0)
    def _():
        pl.semaphore_signal(y_ready, inc=1, device_id={"gy": other_y}, device_id_type=MESH)

    def v_copy(i, a, g, target, send_sem):
        to_a, to_g, pairs = V_COPIES[i]
        return pltpu.make_async_remote_copy(
            src_ref=field.at[a, pl.ds(2 * g, pairs)],
            dst_ref=field.at[to_a, pl.ds(2 * to_g, pairs)],
            send_sem=send_sem.at[i],
            recv_sem=v_recv.at[i],
            device_id=target,
            device_id_type=MESH,
        )

    def e_copy(i, a, g, target, send_sem):
        to_a, to_g, first, last = E_COPIES[i]
        return pltpu.make_async_remote_copy(
            src_ref=edge.at[a, g, pl.ds(first, last - first)],
            dst_ref=edge.at[to_a, to_g, pl.ds(first, last - first)],
            send_sem=send_sem.at[i],
            recv_sem=e_recv.at[i],
            device_id=target,
            device_id_type=MESH,
        )

    slots = [(a, g) for g in range(3) for a in range(3) if a or g]
    copies = {slot: [] for slot in slots}
    to_next = {slot: [] for slot in slots}
    to_second = {slot: [] for slot in slots}
    for make, table, own_sem, next_sem, second_sem in (
        (e_copy, E_COPIES, e_send, e_next, e_second),
        (v_copy, V_COPIES, v_send, v_next, v_second),
    ):
        for i, entry in enumerate(table):
            a, g = entry[:2]
            copies[a, g].append(make(i, 0, 0, below(a, g), own_sem))
            if g == 2 or (g == 1 and a > 0):
                to_next[a, g - 1].append(make(i, a, g - 1, below(0, 1), next_sem))
            if g == 2 and a > 0:
                to_second[a, 0].append(make(i, a, 0, below(0, 2), second_sem))

    def start(partner):
        for copy in copies[partner]:
            copy.start()

    for a, g in PARTNERS:
        when(
            always(sends(a, g), jnp.logical_not(sends_over_end(a, g))),
            lambda a=a, g=g: start((a, g)),
        )
    for a, g in PARTNERS:

        @pl.when(always(sends(a, g), sends_over_end(a, g)))
        def _():
            pl.semaphore_wait(ready.at[PARTNERS.index((a, g))], 1)
            start((a, g))

    def each(some):
        def start_all():
            for copy in some:
                copy.start()

        return start_all

    def arrived(g):
        for a, slot_g in slots:
            if slot_g == g:
                for copy in copies[a, g]:
                    copy.wait_recv()
                onward = to_next[a, g]
                when(odd if g == 1 else bool(onward), each(onward))
                if to_second[a, g]:
                    when(odd, each(to_second[a, g]))

    def both_halves(a, g):
        value = load(edge, (a, g, 2), 2)
        store(tmp, (), value, 2, pl.ds(0, 4))
        store(tmp, (), value, 2, pl.ds(4, 4))
        return third_row(load(tmp, (), 2))

    def spread(matrix, rows, first):
        return per_element(lambda p: jnp.broadcast_to(p[first : first + 1], (8, 128)), matrix[:rows])

    def change_of_gauge(g):
        previous = None
        for a in (2, 1, 0):
            value = both_halves(a, 0)
            if g == 2:
                if a == 2:
                    value = matmul(value, both_halves(2, 1))
                else:
                    value = matmul(value, both_halves(a, 1))
            if a == 2:
                store(left, (2,), spread(value, 2, 0), 2)
                store(right, (2,), spread(value, 3, 1), 3)
            else:
                store(left, (a,), value[:2], 2)
                after = pick(time == 3, previous, rolled(value, 7))
                store(right, (a,), after, 3)
            previous = spread(value, 3, 0)

    def row_pair(a, g, piece, q):
        low = load(edge, (a, g, piece), 2, pl.ds(2 * q, 1))
        high = load(edge, (a, g, piece), 2, pl.ds(2 * q + 1, 1))
        wide = lambda p: jnp.broadcast_to(p, (8, 128))
        return third_row(per_element(lambda p, s: jnp.where(lower, wide(p), wide(s)), low, high))

    def into_window(value, a, g):
        if g > 0:
            value = third_row(matmul_dagger(value, load(right, (a,), 3)))
            value = matmul(load(left, (a,), 2), value)
        return third_row(value)

    def pair(g, q):
        xp = 2 * g + q
        for a in range(2):
            fix = pick(time == 3, row_pair(a + 1, g, 1, q), unit)
            value = matmul_dagger(load(field, (a, xp), 2), fix)
            store(tiles, (a,), into_window(value, a, g), 3)
        store(tiles, (2,), into_window(row_pair(2, g, 0, q)[:2], 2, g), 3)
        product = load(tiles, (0,), 3)
        store(chain, (0, xp), product, 3)
        for k in range(1, TMAX):
            if k < 4:
                here, after = load(tiles, (0,), 3), load(tiles, (1,), 3)
                factor = pick(time < 4 - k, rolled(here, -k), rolled(after, 4 - k))
            elif k == 4:
                factor = load(tiles, (1,), 3)
            else:
                factor = pick(time < 3, rolled(load(tiles, (1,), 3), -1), load(tiles, (2,), 3))
            product = third_row(matmul(product[:2], factor))
            store(chain, (k, xp), product, 3)

    lane = lax.broadcasted_iota(jnp.int32, (8, 128), 1)

    def correlate(sums, picked):
        def body(u, sums):
            totals = {}
            for c in range(18):
                tile = {}

                def even(m):
                    if m not in tile:
                        tile[m] = chain[u, m, c]
                    return tile[m]

                def turned(m):
                    if ("t", m) not in tile:
                        tile["t", m] = roll(even(m), 4)
                    return tile["t", m]

                def odd(m):
                    if ("o", m) not in tile:
                        tile["o", m] = jnp.where(lower, turned(m), turned(m + 1))
                    return tile["o", m]

                for r, xp in picked:
                    far = odd(xp + r // 2) if r % 2 else even(xp + r // 2)
                    term = even(xp) * far
                    totals[r, xp] = totals[r, xp] + term if (r, xp) in totals else term
            for r, xp in picked:
                total = jnp.sum(totals[r, xp], axis=1, keepdims=True)
                sums = jnp.where(lane == 8 * (2 * (r - 1) + xp) + u, total, sums)
            return sums

        return lax.fori_loop(0, TMAX, body, sums)

    def chains(g):
        def body(q, carry):
            pair(g, q)
            return carry

        lax.fori_loop(0, 2 if g < 2 else 1, body, 0)

    loops = [(r, xp) for r in range(1, RMAX + 1) for xp in range(2)]
    last = [(r, xp) for r, xp in loops if xp + (r + 1) // 2 == 4]
    arrived(0)
    change_of_gauge(1)
    chains(0)
    arrived(1)
    chains(1)
    change_of_gauge(2)
    sums = correlate(zero, [loop for loop in loops if loop not in last])
    arrived(2)
    chains(2)
    part[...] = correlate(sums, last)

    for a, g in PARTNERS:

        def sent(a=a, g=g):
            for copy in copies[a, g]:
                copy.wait_send()

        when(sends(a, g), sent)

    for slot in slots:

        def relayed(some):
            def wait_all():
                for copy in some:
                    copy.wait_send()

            return wait_all

        if to_next[slot]:
            when(odd if slot[1] == 1 else True, relayed(to_next[slot]))
        if to_second[slot]:
            when(odd, relayed(to_second[slot]))

    swap = pltpu.make_async_remote_copy(
        src_ref=part,
        dst_ref=peer,
        send_sem=sum_send,
        recv_sem=sum_recv,
        device_id={"gy": other_y},
        device_id_type=MESH,
    )

    @pl.when(y_at == 0)
    def _():
        pl.semaphore_wait(y_ready, 1)

    swap.start()
    swap.wait()
    sums = (part[...] + peer[...]) / (3.0 * 128 * n_y)
    for r, xp in loops:
        at = 8 * (2 * (r - 1) + xp)
        value = sums if at == 0 else pltpu.roll(sums, 128 - at, 1)
        out[r - 1, 2 * xp] = value[0:4, 0:TMAX]
        out[r - 1, 2 * xp + 1] = value[4:8, 0:TMAX]


def solution(mesh):
    sizes = tuple(mesh.shape[name] for name in ("gx", "gy", "ta"))

    def local(link_x, link_t):
        vmem = lambda *shape: pltpu.VMEM(shape, jnp.float32)
        sums = pl.pallas_call(
            lambda *refs: kernel(sizes, *refs),
            out_shape=pltpu.VMEM((RMAX, 4, 4, TMAX), jnp.float32),
            in_specs=[pl.BlockSpec(memory_space=pl.ANY)] * 2,
            out_specs=pl.BlockSpec(memory_space=pltpu.VMEM),
            scratch_shapes=[
                vmem(18, 16, 128),
                vmem(18, 16, 128),
                vmem(2, 5, 12, 8, 128),
                vmem(3, 3, 3, 12, 4, 128),
                vmem(3, 12, 8, 128),
                vmem(3, 18, 8, 128),
                vmem(3, 18, 8, 128),
                vmem(TMAX, 5, 18, 8, 128),
                vmem(12, 8, 128),
                vmem(8, 128),
                vmem(8, 128),
                pltpu.SemaphoreType.DMA((2,)),
                pltpu.SemaphoreType.REGULAR((len(PARTNERS),)),
                pltpu.SemaphoreType.REGULAR,
                pltpu.SemaphoreType.DMA((len(V_COPIES),)),
                pltpu.SemaphoreType.DMA((len(V_COPIES),)),
                pltpu.SemaphoreType.DMA((len(V_COPIES),)),
                pltpu.SemaphoreType.DMA((len(V_COPIES),)),
                pltpu.SemaphoreType.DMA((len(E_COPIES),)),
                pltpu.SemaphoreType.DMA((len(E_COPIES),)),
                pltpu.SemaphoreType.DMA((len(E_COPIES),)),
                pltpu.SemaphoreType.DMA((len(E_COPIES),)),
                pltpu.SemaphoreType.DMA,
                pltpu.SemaphoreType.DMA,
            ],
            compiler_params=pltpu.CompilerParams(collective_id=0, has_side_effects=True),
        )(link_x.reshape(18, 16, 128), link_t.reshape(18, 16, 128))
        return sums.transpose(0, 3, 1, 2)

    return jax.shard_map(
        local,
        mesh=mesh,
        in_specs=(P(None, None, None, "gx", "ta", "gy"),) * 2,
        out_specs=P(None, None, "gx", "ta"),
        check_vma=False,
    )
```

```python
import jax
import jax.numpy as jnp
from jax import lax
from jax.experimental import pallas as pl
from jax.experimental.pallas import tpu as pltpu
from jax.sharding import PartitionSpec as P

RMAX = 6
TMAX = 6
MESH = pl.DeviceIdType.MESH

V_COPIES = ((1, 0, 0), (1, 0, 1), (0, 1, 0), (0, 1, 1), (1, 1, 0), (1, 1, 1), (0, 2, 0), (1, 2, 0))
E_COPIES = (
    (1, 0, 1, 3),
    (2, 0, 0, 3),
    (0, 1, 2, 3),
    (1, 1, 1, 3),
    (2, 1, 0, 3),
    (1, 2, 1, 2),
    (2, 2, 0, 2),
)
PARTNERS = ((0, 1), (0, 2), (1, 0), (2, 0))
ORDER = (
    ("E", 1, 0),
    ("E", 2, 0),
    ("V", 0, 1, 0),
    ("V", 1, 0, 0),
    ("V", 0, 2, 0),
    ("V", 1, 0, 1),
    ("V", 0, 1, 1),
    ("E", 0, 1),
)


def cmul(a, b):
    return a[0] * b[0] - a[1] * b[1], a[0] * b[1] + a[1] * b[0]


def cmul_conj(a, b):
    return a[0] * b[0] + a[1] * b[1], a[1] * b[0] - a[0] * b[1]


def csum(terms):
    real, imag = terms[0]
    for term in terms[1:]:
        real, imag = real + term[0], imag + term[1]
    return real, imag


def matmul(a, b):
    return [[csum([cmul(row[j], b[j][k]) for j in range(3)]) for k in range(3)] for row in a]


def matmul_dagger(a, b):
    return [[csum([cmul_conj(row[j], b[k][j]) for j in range(3)]) for k in range(3)] for row in a]


def third_row(a):
    row = []
    for i in range(3):
        j, k = (i + 1) % 3, (i + 2) % 3
        first = cmul(a[0][j], a[1][k])
        second = cmul(a[0][k], a[1][j])
        row.append((first[0] - second[0], second[1] - first[1]))
    return [a[0], a[1], row]


def per_element(function, *matrices):
    return [
        [tuple(function(*(m[i][j][c] for m in matrices)) for c in range(2)) for j in range(3)]
        for i in range(len(matrices[0]))
    ]


def load(ref, lead, rows, window=slice(None)):
    return [
        [tuple(ref[(*lead, c * 3 * rows + i * 3 + j, window)] for c in range(2)) for j in range(3)]
        for i in range(rows)
    ]


def store(ref, lead, matrix, rows, window=slice(None)):
    for c in range(2):
        for i in range(rows):
            for j in range(3):
                ref[(*lead, c * 3 * rows + i * 3 + j, window)] = matrix[i][j][c]


def roll(value, shift):
    shift = shift % 8
    return value if shift == 0 else pltpu.roll(value, shift, 0)


def kernel(
    sizes, link_x, link_t, out, ux, ut, field, edge, left, right, tiles, chain, tmp, part, peer,
    in_sem, ready, y_ready, v_send, v_recv, v_next, v_second,
    e_send, e_recv, e_next, e_second, sum_send, sum_recv,
):
    n_x, n_y, n_t = sizes
    x_at, y_at, t_at = lax.axis_index("gx"), lax.axis_index("gy"), lax.axis_index("ta")
    other_y = lax.rem(y_at + 1, n_y)

    def above(a, g):
        return {"gx": lax.rem(x_at + g, n_x), "ta": lax.rem(t_at + a, n_t)}

    def below(a, g):
        return {"gx": lax.rem(x_at + n_x - g, n_x), "ta": lax.rem(t_at + n_t - a, n_t)}

    barrier = pltpu.get_barrier_semaphore()
    def always(*conditions):
        known = [c for c in conditions if isinstance(c, bool)]
        traced = [c for c in conditions if not isinstance(c, bool)]
        if not all(known):
            return False
        result = True
        for c in traced:
            result = c if result is True else result & c
        return result

    def when(condition, action):
        if condition is True:
            action()
        elif condition is not False:
            pl.when(condition)(action)

    odd = lax.rem(x_at, 2) == 1

    def sends(a, g):
        return odd if g == 2 else True

    def receives(a, g):
        return odd if g == 2 else True

    def sends_over_end(a, g):
        return (t_at < a) | (x_at < g)

    def receives_over_end(a, g):
        return (t_at + a >= n_t) | (x_at + g >= n_x)

    peers = (y_at > 0).astype(jnp.int32)
    for a, g in PARTNERS:

        @pl.when(always(receives(a, g), jnp.logical_not(receives_over_end(a, g))))
        def _():
            pl.semaphore_signal(barrier, inc=1, device_id=above(a, g), device_id_type=MESH)

        @pl.when(always(sends(a, g), sends_over_end(a, g)))
        def _():
            pl.semaphore_signal(barrier, inc=1, device_id=below(a, g), device_id_type=MESH)

        peers += always(sends(a, g), jnp.logical_not(sends_over_end(a, g))).astype(jnp.int32)
        peers += always(receives(a, g), receives_over_end(a, g)).astype(jnp.int32)

    @pl.when(y_at == 0)
    def _():
        pl.semaphore_signal(barrier, inc=1, device_id={"gy": other_y}, device_id_type=MESH)

    copy_x = pltpu.make_async_copy(link_x, ux, in_sem.at[0])
    copy_t = pltpu.make_async_copy(link_t, ut, in_sem.at[1])
    copy_x.start()
    copy_t.start()

    def enter():
        @pl.when(peers > 0)
        def _():
            pl.semaphore_wait(barrier, peers)

        for k, (a, g) in enumerate(PARTNERS):

            @pl.when(always(receives(a, g), receives_over_end(a, g)))
            def _():
                pl.semaphore_signal(ready.at[k], inc=1, device_id=above(a, g), device_id_type=MESH)

        @pl.when(y_at > 0)
        def _():
            pl.semaphore_signal(y_ready, inc=1, device_id={"gy": other_y}, device_id_type=MESH)

    late = (t_at + 2 >= n_t) | (x_at + 2 >= n_x)

    @pl.when(late)
    def _():
        enter()

    row = lax.broadcasted_iota(jnp.int32, (8, 128), 0)
    time = lax.rem(row, 4)
    lower = row < 4
    one = jnp.ones((8, 128), jnp.float32)
    zero = jnp.zeros((8, 128), jnp.float32)
    unit = [[(one if i == k else zero, zero) for k in range(3)] for i in range(3)]

    def pick(mask, a, b):
        return per_element(lambda p, q: jnp.where(mask, p, q), a, b)

    def rolled(a, shift):
        return per_element(lambda p: roll(p, shift), a)

    copy_x.wait()
    u0 = load(ux, (), 3, pl.ds(0, 8))
    u1 = load(ux, (), 3, pl.ds(8, 8))
    halves = matmul(pick(lower, u0, rolled(u1, 4)), pick(lower, rolled(u0, 4), u1))
    whole = matmul(pick(lower, halves, rolled(halves, 4)), pick(lower, u1, halves))
    starts = [
        pick(lower, unit, rolled(u0, 4)),
        pick(lower, halves, rolled(whole, 4)),
    ]
    store(edge, (0, 0, 2), per_element(lambda p: p[4:8], whole[:2]), 2)
    copy_t.wait()
    links = []
    for xp in range(2):
        begin = starts[xp]
        end = pick(time == 3, unit, rolled(begin, 7))
        v = matmul_dagger(matmul(begin[:2], load(ut, (), 3, pl.ds(8 * xp, 8))), end)
        store(field, (0, xp), v, 2)
        links.append(v)

    def first_times(low, high):
        value = jnp.where(row == 0, low, roll(low, -3))
        value = jnp.where(row == 2, roll(high, 2), value)
        return jnp.where(row == 3, roll(high, -1), value)[0:4]

    store(edge, (0, 0, 0), per_element(first_times, links[0], links[1]), 2)
    store(edge, (0, 0, 1), per_element(first_times, starts[0][:2], starts[1][:2]), 2)


    @pl.when(jnp.logical_not(late))
    def _():
        enter()

    def v_copy(i, a, g, target, send_sem):
        to_a, to_g, pair = V_COPIES[i]
        return pltpu.make_async_remote_copy(
            src_ref=field.at[a, 2 * g + pair],
            dst_ref=field.at[to_a, 2 * to_g + pair],
            send_sem=send_sem.at[i],
            recv_sem=v_recv.at[i],
            device_id=target,
            device_id_type=MESH,
        )

    def e_copy(i, a, g, target, send_sem):
        to_a, to_g, first, last = E_COPIES[i]
        return pltpu.make_async_remote_copy(
            src_ref=edge.at[a, g, pl.ds(first, last - first)],
            dst_ref=edge.at[to_a, to_g, pl.ds(first, last - first)],
            send_sem=send_sem.at[i],
            recv_sem=e_recv.at[i],
            device_id=target,
            device_id_type=MESH,
        )

    copies, to_next, to_second = {}, {}, {}
    for name, make, table, own_sem, next_sem, second_sem in (
        ("E", e_copy, E_COPIES, e_send, e_next, e_second),
        ("V", v_copy, V_COPIES, v_send, v_next, v_second),
    ):
        for i, entry in enumerate(table):
            a, g = entry[:2]
            tile = entry[2:] if name == "V" else ()
            copies[(name, a, g, *tile)] = make(i, 0, 0, below(a, g), own_sem)
            if g == 2 or (g == 1 and a > 0):
                to_next[(name, a, g - 1, *tile)] = make(i, a, g - 1, below(0, 1), next_sem)
            if g == 2 and a > 0:
                to_second[(name, a, 0, *tile)] = make(i, a, 0, below(0, 2), second_sem)

    def start(*partners):
        for key in ORDER:
            if key[1:3] in partners:
                copies[key].start()

    for key in ORDER:
        a, g = key[1:3]
        when(always(sends(a, g), jnp.logical_not(sends_over_end(a, g))), copies[key].start)

    def send_over_end(*partners):
        for a, g in partners:

            @pl.when(always(sends(a, g), sends_over_end(a, g)))
            def _():
                pl.semaphore_wait(ready.at[PARTNERS.index((a, g))], 1)
                start((a, g))

    def take(*keys):
        for key in keys:
            copies[key].wait_recv()
            if key in to_next:
                when(odd if key[2] == 1 else True, to_next[key].start)
            if key in to_second:
                when(odd, to_second[key].start)

    def both_halves(a, g):
        value = load(edge, (a, g, 2), 2)
        store(tmp, (), value, 2, pl.ds(0, 4))
        store(tmp, (), value, 2, pl.ds(4, 4))
        return third_row(load(tmp, (), 2))

    def spread(matrix, rows, first):
        return per_element(lambda p: jnp.broadcast_to(p[first : first + 1], (8, 128)), matrix[:rows])

    def change_of_gauge(g):
        previous = None
        for a in (2, 1, 0):
            value = both_halves(a, 0)
            if g == 2:
                if a == 2:
                    value = matmul(value, both_halves(2, 1))
                else:
                    value = matmul(value, both_halves(a, 1))
            if a == 2:
                store(left, (g - 1, 2), spread(value, 2, 0), 2)
                store(right, (g - 1, 2), spread(value, 3, 1), 3)
            else:
                store(left, (g - 1, a), value[:2], 2)
                after = pick(time == 3, previous, rolled(value, 7))
                store(right, (g - 1, a), after, 3)
            previous = spread(value, 3, 0)

    def row_pair(a, g, piece, q):
        low = load(edge, (a, g, piece), 2, pl.ds(2 * q, 1))
        high = load(edge, (a, g, piece), 2, pl.ds(2 * q + 1, 1))
        wide = lambda p: jnp.broadcast_to(p, (8, 128))
        return third_row(per_element(lambda p, s: jnp.where(lower, wide(p), wide(s)), low, high))

    def into_window(value, a, g):
        if g > 0:
            value = third_row(matmul_dagger(value, load(right, (g - 1, a), 3)))
            value = matmul(load(left, (g - 1, a), 2), value)
        return third_row(value)

    def pair(g, q):
        xp = 2 * g + q
        for a in range(2):
            fix = pick(time == 3, row_pair(a + 1, g, 1, q), unit)
            value = matmul_dagger(load(field, (a, xp), 2), fix)
            store(tiles, (a,), into_window(value, a, g), 3)
        store(tiles, (2,), into_window(row_pair(2, g, 0, q)[:2], 2, g), 3)
        product = load(tiles, (0,), 3)
        store(chain, (0, xp), product, 3)
        for k in range(1, TMAX):
            if k < 4:
                here, after = load(tiles, (0,), 3), load(tiles, (1,), 3)
                factor = pick(time < 4 - k, rolled(here, -k), rolled(after, 4 - k))
            elif k == 4:
                factor = load(tiles, (1,), 3)
            else:
                factor = pick(time < 3, rolled(load(tiles, (1,), 3), -1), load(tiles, (2,), 3))
            product = third_row(matmul(product[:2], factor))
            store(chain, (k, xp), product, 3)

    lane = lax.broadcasted_iota(jnp.int32, (8, 128), 1)

    def correlate(sums, picked):
        def body(u, sums):
            totals = {}
            for c in range(18):
                tile = {}

                def even(m):
                    if m not in tile:
                        tile[m] = chain[u, m, c]
                    return tile[m]

                def turned(m):
                    if ("t", m) not in tile:
                        tile["t", m] = roll(even(m), 4)
                    return tile["t", m]

                def odd(m):
                    if ("o", m) not in tile:
                        tile["o", m] = jnp.where(lower, turned(m), turned(m + 1))
                    return tile["o", m]

                for r, xp in picked:
                    far = odd(xp + r // 2) if r % 2 else even(xp + r // 2)
                    term = even(xp) * far
                    totals[r, xp] = totals[r, xp] + term if (r, xp) in totals else term
            for r, xp in picked:
                total = jnp.sum(totals[r, xp], axis=1, keepdims=True)
                sums = jnp.where(lane == 8 * (2 * (r - 1) + xp) + u, total, sums)
            return sums

        return lax.fori_loop(0, TMAX, body, sums)

    def chains(g, first, end):
        def body(q, carry):
            pair(g, q)
            return carry

        lax.fori_loop(first, end, body, 0)

    loops = [(r, xp) for r in range(1, RMAX + 1) for xp in range(2)]

    def reaching(m):
        return [(r, xp) for r, xp in loops if xp + (r + 1) // 2 == m]

    send_over_end((0, 1), (0, 2))
    take(("E", 1, 0), ("V", 1, 0, 0),)
    send_over_end((2, 0), (1, 0))
    take(("E", 2, 0), ("V", 1, 0, 1),)
    change_of_gauge(1)
    chains(0, 0, 2)
    sums = correlate(zero, reaching(1))
    take(("V", 0, 1, 0), ("E", 1, 1), ("E", 2, 1), ("V", 1, 1, 0))
    chains(1, 0, 1)
    sums = correlate(sums, reaching(2))
    take(("E", 0, 1),)
    change_of_gauge(2)
    take(("V", 0, 1, 1), ("V", 1, 1, 1))
    chains(1, 1, 2)
    sums = correlate(sums, reaching(3))
    take(("E", 1, 2), ("E", 2, 2), ("V", 0, 2, 0), ("V", 1, 2, 0))
    chains(2, 0, 1)
    part[...] = correlate(sums, reaching(4))

    for key in ORDER:
        when(sends(*key[1:3]), copies[key].wait_send)
    for key, copy in to_next.items():
        when(odd if key[2] == 1 else True, copy.wait_send)
    for copy in to_second.values():
        when(odd, copy.wait_send)
    swap = pltpu.make_async_remote_copy(
        src_ref=part,
        dst_ref=peer,
        send_sem=sum_send,
        recv_sem=sum_recv,
        device_id={"gy": other_y},
        device_id_type=MESH,
    )

    @pl.when(y_at == 0)
    def _():
        pl.semaphore_wait(y_ready, 1)

    swap.start()
    swap.wait()
    sums = (part[...] + peer[...]) / (3.0 * 128 * n_y)
    for r, xp in loops:
        at = 8 * (2 * (r - 1) + xp)
        value = sums if at == 0 else pltpu.roll(sums, 128 - at, 1)
        out[r - 1, 2 * xp] = value[0:4, 0:TMAX]
        out[r - 1, 2 * xp + 1] = value[4:8, 0:TMAX]


def solution(mesh):
    sizes = tuple(mesh.shape[name] for name in ("gx", "gy", "ta"))

    def local(link_x, link_t):
        vmem = lambda *shape: pltpu.VMEM(shape, jnp.float32)
        sums = pl.pallas_call(
            lambda *refs: kernel(sizes, *refs),
            out_shape=pltpu.VMEM((RMAX, 4, 4, TMAX), jnp.float32),
            in_specs=[pl.BlockSpec(memory_space=pl.ANY)] * 2,
            out_specs=pl.BlockSpec(memory_space=pltpu.VMEM),
            scratch_shapes=[
                vmem(18, 16, 128),
                vmem(18, 16, 128),
                vmem(2, 5, 12, 8, 128),
                vmem(3, 3, 3, 12, 4, 128),
                vmem(2, 3, 12, 8, 128),
                vmem(2, 3, 18, 8, 128),
                vmem(3, 18, 8, 128),
                vmem(TMAX, 5, 18, 8, 128),
                vmem(12, 8, 128),
                vmem(8, 128),
                vmem(8, 128),
                pltpu.SemaphoreType.DMA((2,)),
                pltpu.SemaphoreType.REGULAR((len(PARTNERS),)),
                pltpu.SemaphoreType.REGULAR,
                pltpu.SemaphoreType.DMA((len(V_COPIES),)),
                pltpu.SemaphoreType.DMA((len(V_COPIES),)),
                pltpu.SemaphoreType.DMA((len(V_COPIES),)),
                pltpu.SemaphoreType.DMA((len(V_COPIES),)),
                pltpu.SemaphoreType.DMA((len(E_COPIES),)),
                pltpu.SemaphoreType.DMA((len(E_COPIES),)),
                pltpu.SemaphoreType.DMA((len(E_COPIES),)),
                pltpu.SemaphoreType.DMA((len(E_COPIES),)),
                pltpu.SemaphoreType.DMA,
                pltpu.SemaphoreType.DMA,
            ],
            compiler_params=pltpu.CompilerParams(collective_id=0, has_side_effects=True),
        )(link_x.reshape(18, 16, 128), link_t.reshape(18, 16, 128))
        return sums.transpose(0, 3, 1, 2)

    return jax.shard_map(
        local,
        mesh=mesh,
        in_specs=(P(None, None, None, "gx", "ta", "gy"),) * 2,
        out_specs=P(None, None, "gx", "ta"),
        check_vma=False,
    )
```

```python
import jax
import jax.numpy as jnp
from jax import lax
from jax.experimental import pallas as pl
from jax.experimental.pallas import tpu as pltpu
from jax.sharding import PartitionSpec as P

RMAX = 6
TMAX = 6
MESH = pl.DeviceIdType.MESH

V_COPIES = ((1, 0, 0), (1, 0, 1), (0, 1, 0), (0, 1, 1), (1, 1, 0), (1, 1, 1), (0, 2, 0), (1, 2, 0))
E_COPIES = (
    (1, 0, 1, 3),
    (2, 0, 0, 3),
    (0, 1, 2, 3),
    (1, 1, 1, 3),
    (2, 1, 0, 3),
    (1, 2, 1, 2),
    (2, 2, 0, 2),
)
PARTNERS = ((0, 1), (0, 2), (1, 0), (2, 0))
ORDER = (
    ("E", 1, 0),
    ("E", 2, 0),
    ("V", 0, 1, 0),
    ("V", 1, 0, 0),
    ("V", 0, 2, 0),
    ("V", 1, 0, 1),
    ("V", 0, 1, 1),
    ("E", 0, 1),
)


def cmul(a, b):
    return a[0] * b[0] - a[1] * b[1], a[0] * b[1] + a[1] * b[0]


def cmul_conj(a, b):
    return a[0] * b[0] + a[1] * b[1], a[1] * b[0] - a[0] * b[1]


def csum(terms):
    real, imag = terms[0]
    for term in terms[1:]:
        real, imag = real + term[0], imag + term[1]
    return real, imag


def matmul(a, b):
    return [[csum([cmul(row[j], b[j][k]) for j in range(3)]) for k in range(3)] for row in a]


def matmul_dagger(a, b):
    return [[csum([cmul_conj(row[j], b[k][j]) for j in range(3)]) for k in range(3)] for row in a]


def third_row(a):
    row = []
    for i in range(3):
        j, k = (i + 1) % 3, (i + 2) % 3
        first = cmul(a[0][j], a[1][k])
        second = cmul(a[0][k], a[1][j])
        row.append((first[0] - second[0], second[1] - first[1]))
    return [a[0], a[1], row]


def per_element(function, *matrices):
    return [
        [tuple(function(*(m[i][j][c] for m in matrices)) for c in range(2)) for j in range(3)]
        for i in range(len(matrices[0]))
    ]


def load(ref, lead, rows, window=slice(None)):
    return [
        [tuple(ref[(*lead, c * 3 * rows + i * 3 + j, window)] for c in range(2)) for j in range(3)]
        for i in range(rows)
    ]


def store(ref, lead, matrix, rows, window=slice(None)):
    for c in range(2):
        for i in range(rows):
            for j in range(3):
                ref[(*lead, c * 3 * rows + i * 3 + j, window)] = matrix[i][j][c]


def roll(value, shift):
    shift = shift % 8
    return value if shift == 0 else pltpu.roll(value, shift, 0)


def kernel(
    sizes, link_x, link_t, out, ux, ut, field, edge, left, right, tiles, chain, tmp, part, peer,
    in_sem, ready, y_ready, v_send, v_recv, v_next, v_second,
    e_send, e_recv, e_next, e_second, sum_send, sum_recv,
):
    n_x, n_y, n_t = sizes
    x_at, y_at, t_at = lax.axis_index("gx"), lax.axis_index("gy"), lax.axis_index("ta")
    other_y = lax.rem(y_at + 1, n_y)

    def above(a, g):
        return {"gx": lax.rem(x_at + g, n_x), "ta": lax.rem(t_at + a, n_t)}

    def below(a, g):
        return {"gx": lax.rem(x_at + n_x - g, n_x), "ta": lax.rem(t_at + n_t - a, n_t)}

    barrier = pltpu.get_barrier_semaphore()
    def always(*conditions):
        known = [c for c in conditions if isinstance(c, bool)]
        traced = [c for c in conditions if not isinstance(c, bool)]
        if not all(known):
            return False
        result = True
        for c in traced:
            result = c if result is True else result & c
        return result

    def when(condition, action):
        if condition is True:
            action()
        elif condition is not False:
            pl.when(condition)(action)

    odd = lax.rem(x_at, 2) == 1

    def sends(a, g):
        return odd if g == 2 else True

    def receives(a, g):
        return odd if g == 2 else True

    def sends_over_end(a, g):
        return (t_at < a) | (x_at < g)

    def receives_over_end(a, g):
        return (t_at + a >= n_t) | (x_at + g >= n_x)

    peers = (y_at > 0).astype(jnp.int32)
    for a, g in PARTNERS:

        @pl.when(always(receives(a, g), jnp.logical_not(receives_over_end(a, g))))
        def _():
            pl.semaphore_signal(barrier, inc=1, device_id=above(a, g), device_id_type=MESH)

        @pl.when(always(sends(a, g), sends_over_end(a, g)))
        def _():
            pl.semaphore_signal(barrier, inc=1, device_id=below(a, g), device_id_type=MESH)

        peers += always(sends(a, g), jnp.logical_not(sends_over_end(a, g))).astype(jnp.int32)
        peers += always(receives(a, g), receives_over_end(a, g)).astype(jnp.int32)

    @pl.when(y_at == 0)
    def _():
        pl.semaphore_signal(barrier, inc=1, device_id={"gy": other_y}, device_id_type=MESH)

    copy_x = pltpu.make_async_copy(link_x, ux, in_sem.at[0])
    copy_t = pltpu.make_async_copy(link_t, ut, in_sem.at[1])
    copy_x.start()
    copy_t.start()

    def enter():
        @pl.when(peers > 0)
        def _():
            pl.semaphore_wait(barrier, peers)

        for k, (a, g) in enumerate(PARTNERS):

            @pl.when(always(receives(a, g), receives_over_end(a, g)))
            def _():
                pl.semaphore_signal(ready.at[k], inc=1, device_id=above(a, g), device_id_type=MESH)

        @pl.when(y_at > 0)
        def _():
            pl.semaphore_signal(y_ready, inc=1, device_id={"gy": other_y}, device_id_type=MESH)

    late = (t_at + 2 >= n_t) | (x_at + 2 >= n_x)

    @pl.when(late)
    def _():
        enter()

    row = lax.broadcasted_iota(jnp.int32, (8, 128), 0)
    time = lax.rem(row, 4)
    lower = row < 4
    one = jnp.ones((8, 128), jnp.float32)
    zero = jnp.zeros((8, 128), jnp.float32)
    unit = [[(one if i == k else zero, zero) for k in range(3)] for i in range(3)]

    def pick(mask, a, b):
        return per_element(lambda p, q: jnp.where(mask, p, q), a, b)

    def rolled(a, shift):
        return per_element(lambda p: roll(p, shift), a)

    copy_x.wait()
    u0 = load(ux, (), 3, pl.ds(0, 8))
    u1 = load(ux, (), 3, pl.ds(8, 8))
    halves = matmul(pick(lower, u0, rolled(u1, 4)), pick(lower, rolled(u0, 4), u1))
    whole = matmul(pick(lower, halves, rolled(halves, 4)), pick(lower, u1, halves))
    starts = [
        pick(lower, unit, rolled(u0, 4)),
        pick(lower, halves, rolled(whole, 4)),
    ]
    store(edge, (0, 0, 2), per_element(lambda p: p[4:8], whole[:2]), 2)
    copy_t.wait()
    links = []
    for xp in range(2):
        begin = starts[xp]
        end = pick(time == 3, unit, rolled(begin, 7))
        v = matmul_dagger(matmul(begin[:2], load(ut, (), 3, pl.ds(8 * xp, 8))), end)
        store(field, (0, xp), v, 2)
        links.append(v)

    def first_times(low, high):
        value = jnp.where(row == 0, low, roll(low, -3))
        value = jnp.where(row == 2, roll(high, 2), value)
        return jnp.where(row == 3, roll(high, -1), value)[0:4]

    store(edge, (0, 0, 0), per_element(first_times, links[0], links[1]), 2)
    store(edge, (0, 0, 1), per_element(first_times, starts[0][:2], starts[1][:2]), 2)


    @pl.when(jnp.logical_not(late))
    def _():
        enter()

    def v_copy(i, a, g, target, send_sem):
        to_a, to_g, pair = V_COPIES[i]
        return pltpu.make_async_remote_copy(
            src_ref=field.at[a, 2 * g + pair],
            dst_ref=field.at[to_a, 2 * to_g + pair],
            send_sem=send_sem.at[i],
            recv_sem=v_recv.at[i],
            device_id=target,
            device_id_type=MESH,
        )

    def e_copy(i, a, g, target, send_sem):
        to_a, to_g, first, last = E_COPIES[i]
        return pltpu.make_async_remote_copy(
            src_ref=edge.at[a, g, pl.ds(first, last - first)],
            dst_ref=edge.at[to_a, to_g, pl.ds(first, last - first)],
            send_sem=send_sem.at[i],
            recv_sem=e_recv.at[i],
            device_id=target,
            device_id_type=MESH,
        )

    copies, to_next, to_second = {}, {}, {}
    for name, make, table, own_sem, next_sem, second_sem in (
        ("E", e_copy, E_COPIES, e_send, e_next, e_second),
        ("V", v_copy, V_COPIES, v_send, v_next, v_second),
    ):
        for i, entry in enumerate(table):
            a, g = entry[:2]
            tile = entry[2:] if name == "V" else ()
            copies[(name, a, g, *tile)] = make(i, 0, 0, below(a, g), own_sem)
            if g == 2 or (g == 1 and a > 0):
                to_next[(name, a, g - 1, *tile)] = make(i, a, g - 1, below(0, 1), next_sem)
            if g == 2 and a > 0:
                to_second[(name, a, 0, *tile)] = make(i, a, 0, below(0, 2), second_sem)

    def start(*partners):
        for key in ORDER:
            if key[1:3] in partners:
                copies[key].start()

    for key in ORDER:
        a, g = key[1:3]
        when(always(sends(a, g), jnp.logical_not(sends_over_end(a, g))), copies[key].start)

    def send_over_end(*partners):
        for a, g in partners:

            @pl.when(always(sends(a, g), sends_over_end(a, g)))
            def _():
                pl.semaphore_wait(ready.at[PARTNERS.index((a, g))], 1)
                start((a, g))

    def take(*keys):
        for key in keys:
            copies[key].wait_recv()
            if key in to_next:
                when(odd if key[2] == 1 else True, to_next[key].start)
            if key in to_second:
                when(odd, to_second[key].start)

    def both_halves(a, g):
        value = load(edge, (a, g, 2), 2)
        store(tmp, (), value, 2, pl.ds(0, 4))
        store(tmp, (), value, 2, pl.ds(4, 4))
        return third_row(load(tmp, (), 2))

    def spread(matrix, rows, first):
        return per_element(lambda p: jnp.broadcast_to(p[first : first + 1], (8, 128)), matrix[:rows])

    def change_of_gauge(g):
        previous = None
        for a in (2, 1, 0):
            value = both_halves(a, 0)
            if g == 2:
                if a == 2:
                    value = matmul(value, both_halves(2, 1))
                else:
                    value = matmul(value, both_halves(a, 1))
            if a == 2:
                store(left, (g - 1, 2), spread(value, 2, 0), 2)
                store(right, (g - 1, 2), spread(value, 3, 1), 3)
            else:
                store(left, (g - 1, a), value[:2], 2)
                after = pick(time == 3, previous, rolled(value, 7))
                store(right, (g - 1, a), after, 3)
            previous = spread(value, 3, 0)

    def row_pair(a, g, piece, q):
        low = load(edge, (a, g, piece), 2, pl.ds(2 * q, 1))
        high = load(edge, (a, g, piece), 2, pl.ds(2 * q + 1, 1))
        wide = lambda p: jnp.broadcast_to(p, (8, 128))
        return third_row(per_element(lambda p, s: jnp.where(lower, wide(p), wide(s)), low, high))

    def into_window(value, a, g):
        if g > 0:
            value = third_row(matmul_dagger(value, load(right, (g - 1, a), 3)))
            value = matmul(load(left, (g - 1, a), 2), value)
        return third_row(value)

    def pair(g, q):
        xp = 2 * g + q
        for a in range(2):
            fix = pick(time == 3, row_pair(a + 1, g, 1, q), unit)
            value = matmul_dagger(load(field, (a, xp), 2), fix)
            store(tiles, (a,), into_window(value, a, g), 3)
        store(tiles, (2,), into_window(row_pair(2, g, 0, q)[:2], 2, g), 3)
        product = load(tiles, (0,), 3)
        store(chain, (0, xp), product, 3)
        for k in range(1, TMAX):
            if k < 4:
                here, after = load(tiles, (0,), 3), load(tiles, (1,), 3)
                factor = pick(time < 4 - k, rolled(here, -k), rolled(after, 4 - k))
            elif k == 4:
                factor = load(tiles, (1,), 3)
            else:
                factor = pick(time < 3, rolled(load(tiles, (1,), 3), -1), load(tiles, (2,), 3))
            product = third_row(matmul(product[:2], factor))
            store(chain, (k, xp), product, 3)

    lane = lax.broadcasted_iota(jnp.int32, (8, 128), 1)

    def correlate(sums, picked):
        def body(u, sums):
            totals = {}
            for c in range(18):
                tile = {}

                def even(m):
                    if m not in tile:
                        tile[m] = chain[u, m, c]
                    return tile[m]

                def turned(m):
                    if ("t", m) not in tile:
                        tile["t", m] = roll(even(m), 4)
                    return tile["t", m]

                def odd(m):
                    if ("o", m) not in tile:
                        tile["o", m] = jnp.where(lower, turned(m), turned(m + 1))
                    return tile["o", m]

                for r, xp in picked:
                    far = odd(xp + r // 2) if r % 2 else even(xp + r // 2)
                    term = even(xp) * far
                    totals[r, xp] = totals[r, xp] + term if (r, xp) in totals else term
            for r, xp in picked:
                total = jnp.sum(totals[r, xp], axis=1, keepdims=True)
                sums = jnp.where(lane == 8 * (2 * (r - 1) + xp) + u, total, sums)
            return sums

        return lax.fori_loop(0, TMAX, body, sums)

    def chains(g, first, end):
        def body(q, carry):
            pair(g, q)
            return carry

        lax.fori_loop(first, end, body, 0)

    loops = [(r, xp) for r in range(1, RMAX + 1) for xp in range(2)]

    def reaching(m):
        return [(r, xp) for r, xp in loops if xp + (r + 1) // 2 == m]

    send_over_end((0, 1), (0, 2))
    take(("E", 1, 0), ("V", 1, 0, 0),)
    send_over_end((2, 0), (1, 0))
    take(("E", 2, 0), ("V", 1, 0, 1),)
    change_of_gauge(1)
    chains(0, 0, 2)
    sums = correlate(zero, reaching(1))
    take(("V", 0, 1, 0), ("E", 1, 1), ("E", 2, 1), ("V", 1, 1, 0))
    chains(1, 0, 1)
    sums = correlate(sums, reaching(2))
    take(("E", 0, 1),)
    change_of_gauge(2)
    take(("V", 0, 1, 1), ("V", 1, 1, 1))
    chains(1, 1, 2)
    take(("E", 1, 2), ("E", 2, 2), ("V", 0, 2, 0), ("V", 1, 2, 0))
    chains(2, 0, 1)
    part[...] = correlate(sums, reaching(3) + reaching(4))

    swap = pltpu.make_async_remote_copy(
        src_ref=part,
        dst_ref=peer,
        send_sem=sum_send,
        recv_sem=sum_recv,
        device_id={"gy": other_y},
        device_id_type=MESH,
    )

    @pl.when(y_at == 0)
    def _():
        pl.semaphore_wait(y_ready, 1)

    swap.start()
    for key in ORDER:
        when(sends(*key[1:3]), copies[key].wait_send)
    for key, copy in to_next.items():
        when(odd if key[2] == 1 else True, copy.wait_send)
    for copy in to_second.values():
        when(odd, copy.wait_send)
    swap.wait()
    sums = (part[...] + peer[...]) / (3.0 * 128 * n_y)
    for r, xp in loops:
        at = 8 * (2 * (r - 1) + xp)
        value = sums if at == 0 else pltpu.roll(sums, 128 - at, 1)
        out[r - 1, 2 * xp] = value[0:4, 0:TMAX]
        out[r - 1, 2 * xp + 1] = value[4:8, 0:TMAX]


def solution(mesh):
    sizes = tuple(mesh.shape[name] for name in ("gx", "gy", "ta"))

    def local(link_x, link_t):
        vmem = lambda *shape: pltpu.VMEM(shape, jnp.float32)
        sums = pl.pallas_call(
            lambda *refs: kernel(sizes, *refs),
            out_shape=pltpu.VMEM((RMAX, 4, 4, TMAX), jnp.float32),
            in_specs=[pl.BlockSpec(memory_space=pl.ANY)] * 2,
            out_specs=pl.BlockSpec(memory_space=pltpu.VMEM),
            scratch_shapes=[
                vmem(18, 16, 128),
                vmem(18, 16, 128),
                vmem(2, 5, 12, 8, 128),
                vmem(3, 3, 3, 12, 4, 128),
                vmem(2, 3, 12, 8, 128),
                vmem(2, 3, 18, 8, 128),
                vmem(3, 18, 8, 128),
                vmem(TMAX, 5, 18, 8, 128),
                vmem(12, 8, 128),
                vmem(8, 128),
                vmem(8, 128),
                pltpu.SemaphoreType.DMA((2,)),
                pltpu.SemaphoreType.REGULAR((len(PARTNERS),)),
                pltpu.SemaphoreType.REGULAR,
                pltpu.SemaphoreType.DMA((len(V_COPIES),)),
                pltpu.SemaphoreType.DMA((len(V_COPIES),)),
                pltpu.SemaphoreType.DMA((len(V_COPIES),)),
                pltpu.SemaphoreType.DMA((len(V_COPIES),)),
                pltpu.SemaphoreType.DMA((len(E_COPIES),)),
                pltpu.SemaphoreType.DMA((len(E_COPIES),)),
                pltpu.SemaphoreType.DMA((len(E_COPIES),)),
                pltpu.SemaphoreType.DMA((len(E_COPIES),)),
                pltpu.SemaphoreType.DMA,
                pltpu.SemaphoreType.DMA,
            ],
            compiler_params=pltpu.CompilerParams(collective_id=0, has_side_effects=True),
        )(link_x.reshape(18, 16, 128), link_t.reshape(18, 16, 128))
        return sums.transpose(0, 3, 1, 2)

    return jax.shard_map(
        local,
        mesh=mesh,
        in_specs=(P(None, None, None, "gx", "ta", "gy"),) * 2,
        out_specs=P(None, None, "gx", "ta"),
        check_vma=False,
    )
```

```python
import jax
import jax.numpy as jnp
from jax import lax
from jax.experimental import pallas as pl
from jax.experimental.pallas import tpu as pltpu
from jax.sharding import PartitionSpec as P

RMAX = 6
TMAX = 6
MESH = pl.DeviceIdType.MESH

V_COPIES = ((1, 0, 0), (1, 0, 1), (0, 1, 0), (0, 1, 1), (1, 1, 0), (1, 1, 1), (0, 2, 0), (1, 2, 0))
E_COPIES = (
    (1, 0, 1, 3),
    (2, 0, 0, 3),
    (0, 1, 2, 3),
    (1, 1, 1, 3),
    (2, 1, 0, 3),
    (1, 2, 1, 2),
    (2, 2, 0, 2),
)
PARTNERS = ((0, 1), (0, 2), (1, 0), (2, 0))
ORDER = (
    ("E", 1, 0),
    ("E", 2, 0),
    ("V", 0, 1, 0),
    ("V", 1, 0, 0),
    ("V", 0, 2, 0),
    ("V", 1, 0, 1),
    ("V", 0, 1, 1),
    ("E", 0, 1),
)


def cmul(a, b):
    return a[0] * b[0] - a[1] * b[1], a[0] * b[1] + a[1] * b[0]


def cmul_conj(a, b):
    return a[0] * b[0] + a[1] * b[1], a[1] * b[0] - a[0] * b[1]


def csum(terms):
    real, imag = terms[0]
    for term in terms[1:]:
        real, imag = real + term[0], imag + term[1]
    return real, imag


def matmul(a, b):
    return [[csum([cmul(row[j], b[j][k]) for j in range(3)]) for k in range(3)] for row in a]


def matmul_dagger(a, b):
    return [[csum([cmul_conj(row[j], b[k][j]) for j in range(3)]) for k in range(3)] for row in a]


def third_row(a):
    row = []
    for i in range(3):
        j, k = (i + 1) % 3, (i + 2) % 3
        first = cmul(a[0][j], a[1][k])
        second = cmul(a[0][k], a[1][j])
        row.append((first[0] - second[0], second[1] - first[1]))
    return [a[0], a[1], row]


def per_element(function, *matrices):
    return [
        [tuple(function(*(m[i][j][c] for m in matrices)) for c in range(2)) for j in range(3)]
        for i in range(len(matrices[0]))
    ]


def load(ref, lead, rows, window=slice(None)):
    return [
        [tuple(ref[(*lead, c * 3 * rows + i * 3 + j, window)] for c in range(2)) for j in range(3)]
        for i in range(rows)
    ]


def store(ref, lead, matrix, rows, window=slice(None)):
    for c in range(2):
        for i in range(rows):
            for j in range(3):
                ref[(*lead, c * 3 * rows + i * 3 + j, window)] = matrix[i][j][c]


def roll(value, shift):
    shift = shift % 8
    return value if shift == 0 else pltpu.roll(value, shift, 0)


def kernel(
    sizes, link_x, link_t, out, ux, ut, field, edge, left, right, tiles, chain, tmp, part, peer,
    in_sem, ready, y_ready, v_send, v_recv, v_next, v_second,
    e_send, e_recv, e_next, e_second, sum_send, sum_recv,
):
    n_x, n_y, n_t = sizes
    x_at, y_at, t_at = lax.axis_index("gx"), lax.axis_index("gy"), lax.axis_index("ta")
    other_y = lax.rem(y_at + 1, n_y)

    def above(a, g):
        return {"gx": lax.rem(x_at + g, n_x), "ta": lax.rem(t_at + a, n_t)}

    def below(a, g):
        return {"gx": lax.rem(x_at + n_x - g, n_x), "ta": lax.rem(t_at + n_t - a, n_t)}

    barrier = pltpu.get_barrier_semaphore()
    def always(*conditions):
        known = [c for c in conditions if isinstance(c, bool)]
        traced = [c for c in conditions if not isinstance(c, bool)]
        if not all(known):
            return False
        result = True
        for c in traced:
            result = c if result is True else result & c
        return result

    def when(condition, action):
        if condition is True:
            action()
        elif condition is not False:
            pl.when(condition)(action)

    odd = lax.rem(x_at, 2) == 1

    def sends(a, g):
        return odd if g == 2 else True

    def receives(a, g):
        return odd if g == 2 else True

    def sends_over_end(a, g):
        return (t_at < a) | (x_at < g)

    def receives_over_end(a, g):
        return (t_at + a >= n_t) | (x_at + g >= n_x)

    peers = (y_at > 0).astype(jnp.int32)
    for a, g in PARTNERS:

        @pl.when(always(receives(a, g), jnp.logical_not(receives_over_end(a, g))))
        def _():
            pl.semaphore_signal(barrier, inc=1, device_id=above(a, g), device_id_type=MESH)

        @pl.when(always(sends(a, g), sends_over_end(a, g)))
        def _():
            pl.semaphore_signal(barrier, inc=1, device_id=below(a, g), device_id_type=MESH)

        peers += always(sends(a, g), jnp.logical_not(sends_over_end(a, g))).astype(jnp.int32)
        peers += always(receives(a, g), receives_over_end(a, g)).astype(jnp.int32)

    @pl.when(y_at == 0)
    def _():
        pl.semaphore_signal(barrier, inc=1, device_id={"gy": other_y}, device_id_type=MESH)

    copy_x = pltpu.make_async_copy(link_x, ux, in_sem.at[0])
    copy_t = pltpu.make_async_copy(link_t, ut, in_sem.at[1])
    copy_x.start()
    copy_t.start()

    def enter():
        @pl.when(peers > 0)
        def _():
            pl.semaphore_wait(barrier, peers)

        for k, (a, g) in enumerate(PARTNERS):

            @pl.when(always(receives(a, g), receives_over_end(a, g)))
            def _():
                pl.semaphore_signal(ready.at[k], inc=1, device_id=above(a, g), device_id_type=MESH)

        @pl.when(y_at > 0)
        def _():
            pl.semaphore_signal(y_ready, inc=1, device_id={"gy": other_y}, device_id_type=MESH)

    late = (t_at + 2 >= n_t) | (x_at + 2 >= n_x)

    @pl.when(late)
    def _():
        enter()

    row = lax.broadcasted_iota(jnp.int32, (8, 128), 0)
    time = lax.rem(row, 4)
    lower = row < 4
    one = jnp.ones((8, 128), jnp.float32)
    zero = jnp.zeros((8, 128), jnp.float32)
    unit = [[(one if i == k else zero, zero) for k in range(3)] for i in range(3)]

    def pick(mask, a, b):
        return per_element(lambda p, q: jnp.where(mask, p, q), a, b)

    def rolled(a, shift):
        return per_element(lambda p: roll(p, shift), a)

    copy_x.wait()
    u0 = load(ux, (), 3, pl.ds(0, 8))
    u1 = load(ux, (), 3, pl.ds(8, 8))
    halves = matmul(pick(lower, u0, rolled(u1, 4)), pick(lower, rolled(u0, 4), u1))
    whole = matmul(pick(lower, halves, rolled(halves, 4)), pick(lower, u1, halves))
    starts = [
        pick(lower, unit, rolled(u0, 4)),
        pick(lower, halves, rolled(whole, 4)),
    ]
    store(edge, (0, 0, 2), per_element(lambda p: p[4:8], whole[:2]), 2)
    copy_t.wait()
    links = []
    for xp in range(2):
        begin = starts[xp]
        end = pick(time == 3, unit, rolled(begin, 7))
        v = matmul_dagger(matmul(begin[:2], load(ut, (), 3, pl.ds(8 * xp, 8))), end)
        store(field, (0, xp), v, 2)
        links.append(v)

    def first_times(low, high):
        value = jnp.where(row == 0, low, roll(low, -3))
        value = jnp.where(row == 2, roll(high, 2), value)
        return jnp.where(row == 3, roll(high, -1), value)[0:4]

    store(edge, (0, 0, 0), per_element(first_times, links[0], links[1]), 2)
    store(edge, (0, 0, 1), per_element(first_times, starts[0][:2], starts[1][:2]), 2)


    @pl.when(jnp.logical_not(late))
    def _():
        enter()

    def v_copy(i, a, g, target, send_sem):
        to_a, to_g, pair = V_COPIES[i]
        return pltpu.make_async_remote_copy(
            src_ref=field.at[a, 2 * g + pair],
            dst_ref=field.at[to_a, 2 * to_g + pair],
            send_sem=send_sem.at[i],
            recv_sem=v_recv.at[i],
            device_id=target,
            device_id_type=MESH,
        )

    def e_copy(i, a, g, target, send_sem):
        to_a, to_g, first, last = E_COPIES[i]
        return pltpu.make_async_remote_copy(
            src_ref=edge.at[a, g, pl.ds(first, last - first)],
            dst_ref=edge.at[to_a, to_g, pl.ds(first, last - first)],
            send_sem=send_sem.at[i],
            recv_sem=e_recv.at[i],
            device_id=target,
            device_id_type=MESH,
        )

    copies, to_next, to_second = {}, {}, {}
    for name, make, table, own_sem, next_sem, second_sem in (
        ("E", e_copy, E_COPIES, e_send, e_next, e_second),
        ("V", v_copy, V_COPIES, v_send, v_next, v_second),
    ):
        for i, entry in enumerate(table):
            a, g = entry[:2]
            tile = entry[2:] if name == "V" else ()
            copies[(name, a, g, *tile)] = make(i, 0, 0, below(a, g), own_sem)
            if g == 2 or (g == 1 and a > 0):
                to_next[(name, a, g - 1, *tile)] = make(i, a, g - 1, below(0, 1), next_sem)
            if g == 2 and a > 0:
                to_second[(name, a, 0, *tile)] = make(i, a, 0, below(0, 2), second_sem)

    def start(*partners):
        for key in ORDER:
            if key[1:3] in partners:
                copies[key].start()

    for key in ORDER:
        a, g = key[1:3]
        when(always(sends(a, g), jnp.logical_not(sends_over_end(a, g))), copies[key].start)

    def send_over_end(*partners):
        for a, g in partners:

            @pl.when(always(sends(a, g), sends_over_end(a, g)))
            def _():
                pl.semaphore_wait(ready.at[PARTNERS.index((a, g))], 1)
                start((a, g))

    def take(*keys):
        for key in keys:
            copies[key].wait_recv()
            if key in to_next:
                when(odd if key[2] == 1 else True, to_next[key].start)
            if key in to_second:
                when(odd, to_second[key].start)

    def both_halves(a, g):
        value = load(edge, (a, g, 2), 2)
        store(tmp, (), value, 2, pl.ds(0, 4))
        store(tmp, (), value, 2, pl.ds(4, 4))
        return third_row(load(tmp, (), 2))

    def spread(matrix, rows, first):
        return per_element(lambda p: jnp.broadcast_to(p[first : first + 1], (8, 128)), matrix[:rows])

    def change_of_gauge(g):
        previous = None
        for a in (2, 1, 0):
            value = both_halves(a, 0)
            if g == 2:
                if a == 2:
                    value = matmul(value, both_halves(2, 1))
                else:
                    value = matmul(value, both_halves(a, 1))
            if a == 2:
                store(left, (g - 1, 2), spread(value, 2, 0), 2)
                store(right, (g - 1, 2), spread(value, 3, 1), 3)
            else:
                store(left, (g - 1, a), value[:2], 2)
                after = pick(time == 3, previous, rolled(value, 7))
                store(right, (g - 1, a), after, 3)
            previous = spread(value, 3, 0)

    def row_pair(a, g, piece, q):
        low = load(edge, (a, g, piece), 2, pl.ds(2 * q, 1))
        high = load(edge, (a, g, piece), 2, pl.ds(2 * q + 1, 1))
        wide = lambda p: jnp.broadcast_to(p, (8, 128))
        return third_row(per_element(lambda p, s: jnp.where(lower, wide(p), wide(s)), low, high))

    def into_window(value, a, g):
        if g > 0:
            value = third_row(matmul_dagger(value, load(right, (g - 1, a), 3)))
            value = matmul(load(left, (g - 1, a), 2), value)
        return third_row(value)

    def pair(g, q):
        xp = 2 * g + q
        for a in range(2):
            fix = pick(time == 3, row_pair(a + 1, g, 1, q), unit)
            value = matmul_dagger(load(field, (a, xp), 2), fix)
            store(tiles, (a,), into_window(value, a, g), 3)
        store(tiles, (2,), into_window(row_pair(2, g, 0, q)[:2], 2, g), 3)
        product = load(tiles, (0,), 3)
        store(chain, (0, xp), product, 3)
        for k in range(1, TMAX):
            if k < 4:
                here, after = load(tiles, (0,), 3), load(tiles, (1,), 3)
                factor = pick(time < 4 - k, rolled(here, -k), rolled(after, 4 - k))
            elif k == 4:
                factor = load(tiles, (1,), 3)
            else:
                factor = pick(time < 3, rolled(load(tiles, (1,), 3), -1), load(tiles, (2,), 3))
            product = third_row(matmul(product[:2], factor))
            store(chain, (k, xp), product, 3)

    lane = lax.broadcasted_iota(jnp.int32, (8, 128), 1)

    def correlate(sums, picked):
        def body(u, sums):
            totals = {}
            for c in range(18):
                tile = {}

                def even(m):
                    if m not in tile:
                        tile[m] = chain[u, m, c]
                    return tile[m]

                def turned(m):
                    if ("t", m) not in tile:
                        tile["t", m] = roll(even(m), 4)
                    return tile["t", m]

                def odd(m):
                    if ("o", m) not in tile:
                        tile["o", m] = jnp.where(lower, turned(m), turned(m + 1))
                    return tile["o", m]

                for r, xp in picked:
                    far = odd(xp + r // 2) if r % 2 else even(xp + r // 2)
                    term = even(xp) * far
                    totals[r, xp] = totals[r, xp] + term if (r, xp) in totals else term
            for r, xp in picked:
                total = jnp.sum(totals[r, xp], axis=1, keepdims=True)
                sums = jnp.where(lane == 8 * (2 * (r - 1) + xp) + u, total, sums)
            return sums

        return lax.fori_loop(0, TMAX, body, sums)

    def chains(g, first, end):
        def body(q, carry):
            pair(g, q)
            return carry

        lax.fori_loop(first, end, body, 0)

    loops = [(r, xp) for r in range(1, RMAX + 1) for xp in range(2)]

    def reaching(m):
        return [(r, xp) for r, xp in loops if xp + (r + 1) // 2 == m]

    send_over_end((0, 1), (0, 2))
    take(("E", 1, 0), ("V", 1, 0, 0))
    send_over_end((2, 0), (1, 0))
    take(("E", 2, 0),)
    change_of_gauge(1)
    take(("V", 1, 0, 1),)
    chains(0, 0, 2)
    sums = correlate(zero, reaching(1))
    take(("V", 0, 1, 0), ("E", 1, 1), ("E", 2, 1), ("E", 0, 1))
    change_of_gauge(2)
    take(("V", 1, 1, 0),)
    chains(1, 0, 1)
    sums = correlate(sums, reaching(2))
    take(("V", 0, 1, 1), ("V", 1, 1, 1))
    chains(1, 1, 2)
    take(("E", 1, 2), ("E", 2, 2), ("V", 0, 2, 0), ("V", 1, 2, 0))
    chains(2, 0, 1)
    part[...] = correlate(sums, reaching(3) + reaching(4))

    swap = pltpu.make_async_remote_copy(
        src_ref=part,
        dst_ref=peer,
        send_sem=sum_send,
        recv_sem=sum_recv,
        device_id={"gy": other_y},
        device_id_type=MESH,
    )

    @pl.when(y_at == 0)
    def _():
        pl.semaphore_wait(y_ready, 1)

    swap.start()
    for key in ORDER:
        when(sends(*key[1:3]), copies[key].wait_send)
    for key, copy in to_next.items():
        when(odd if key[2] == 1 else True, copy.wait_send)
    for copy in to_second.values():
        when(odd, copy.wait_send)
    swap.wait()
    sums = (part[...] + peer[...]) / (3.0 * 128 * n_y)
    for r, xp in loops:
        at = 8 * (2 * (r - 1) + xp)
        value = sums if at == 0 else pltpu.roll(sums, 128 - at, 1)
        out[r - 1, 2 * xp] = value[0:4, 0:TMAX]
        out[r - 1, 2 * xp + 1] = value[4:8, 0:TMAX]


def solution(mesh):
    sizes = tuple(mesh.shape[name] for name in ("gx", "gy", "ta"))

    def local(link_x, link_t):
        vmem = lambda *shape: pltpu.VMEM(shape, jnp.float32)
        sums = pl.pallas_call(
            lambda *refs: kernel(sizes, *refs),
            out_shape=pltpu.VMEM((RMAX, 4, 4, TMAX), jnp.float32),
            in_specs=[pl.BlockSpec(memory_space=pl.ANY)] * 2,
            out_specs=pl.BlockSpec(memory_space=pltpu.VMEM),
            scratch_shapes=[
                vmem(18, 16, 128),
                vmem(18, 16, 128),
                vmem(2, 5, 12, 8, 128),
                vmem(3, 3, 3, 12, 4, 128),
                vmem(2, 3, 12, 8, 128),
                vmem(2, 3, 18, 8, 128),
                vmem(3, 18, 8, 128),
                vmem(TMAX, 5, 18, 8, 128),
                vmem(12, 8, 128),
                vmem(8, 128),
                vmem(8, 128),
                pltpu.SemaphoreType.DMA((2,)),
                pltpu.SemaphoreType.REGULAR((len(PARTNERS),)),
                pltpu.SemaphoreType.REGULAR,
                pltpu.SemaphoreType.DMA((len(V_COPIES),)),
                pltpu.SemaphoreType.DMA((len(V_COPIES),)),
                pltpu.SemaphoreType.DMA((len(V_COPIES),)),
                pltpu.SemaphoreType.DMA((len(V_COPIES),)),
                pltpu.SemaphoreType.DMA((len(E_COPIES),)),
                pltpu.SemaphoreType.DMA((len(E_COPIES),)),
                pltpu.SemaphoreType.DMA((len(E_COPIES),)),
                pltpu.SemaphoreType.DMA((len(E_COPIES),)),
                pltpu.SemaphoreType.DMA,
                pltpu.SemaphoreType.DMA,
            ],
            compiler_params=pltpu.CompilerParams(collective_id=0, has_side_effects=True),
        )(link_x.reshape(18, 16, 128), link_t.reshape(18, 16, 128))
        return sums.transpose(0, 3, 1, 2)

    return jax.shard_map(
        local,
        mesh=mesh,
        in_specs=(P(None, None, None, "gx", "ta", "gy"),) * 2,
        out_specs=P(None, None, "gx", "ta"),
        check_vma=False,
    )
```
